32 devices in a mesh: dp: 4 (over z), section: 4 (over x, core), head: 2 (over y).
Axes of the slice: x: 2, y: 2, z: 4, core: 2. Of those that a mesh axis runs over, the one named last changes fastest.
Arguments:
- q_latent: bfloat16 [4, 2048, 1536], P('section', 'dp'), may hold values from -6 to 6
- kv_latent: bfloat16 [4, 2048, 576], P('section', 'dp'), may hold values from -6 to 6
- segment_ids: int32 [2048], P('dp'), may hold values from 0 to 31, never falling along the last dimension, each value on 1 to 512 neighbouring positions
- q_weight: bfloat16 [4, 1536, 12288], P('section', 'dp', 'head'), may hold values from -100 to 100
- k_weight: bfloat16 [4, 512, 8192], P('section', None, 'head'), may hold values from -0.25 to 0.25
Outputs:
- logit_ratio: float32 [4, 64], P(None, 'head')
- scaled_q: bfloat16 [4, 1536, 12288], P('section', 'dp', 'head')
- scaled_k: bfloat16 [4, 512, 8192], P('section', None, 'head')
The draws below stay inside these ranges and needn't reach their ends.
All inputs are finite; a program needn't handle non-finite values.
Results may differ from the reference program's by a relative error of at most 0.0034.
Values may be sent and summed in bfloat16 or wider, within the bound.
A program may use at most 128 MiB of HBM per device.

```python
import math
import jax
import jax.numpy as jnp
import numpy as np
from jax import lax

D_Q = 1536
D_KV = 512
NOPE = 128
ROPE = 64
HEADS = 64
SEQ = 512
LAYERS = 4
TOKENS = 2048
N_DP = 4


def draw_q_weight(key, part):
    scale_key, entry_key = jax.random.split(jax.random.fold_in(key, 11))
    head_scale = jnp.exp(jax.random.uniform(scale_key, (LAYERS, 1, HEADS, 1), jnp.float32, math.log(2.0), math.log(100.0)))
    entries = jax.random.normal(entry_key, (LAYERS, D_Q, HEADS, NOPE + ROPE), jnp.float32)
    weights = entries * head_scale / math.sqrt(D_Q)
    return weights.reshape(LAYERS, D_Q, HEADS * (NOPE + ROPE)).astype(jnp.bfloat16)


def level_of(stream_key, dims, cuts, smallest, top_value):
    def one(dim, blocks):
        steps = jax.random.uniform(jax.random.fold_in(jax.random.fold_in(stream_key, 6), dim), (blocks,), jnp.float32, smallest / len(cuts), top_value / len(cuts))
        return jnp.repeat(jnp.exp(steps), dims[dim] // blocks).reshape((-1,) + (1,) * (len(dims) - dim - 1))

    loudness = one(*cuts[0])
    for cut in cuts[1:]:
        loudness = loudness * one(*cut)
    return loudness


def split_up(amount, total, limit, slope):
    loads = [(1 << 20) // math.isqrt(standing ** slope) + 1 for standing in range(2, amount + 1)]
    rest, counts = total - limit - (amount - 1), [1] * (amount - 1)
    while rest > 0:
        free = [i for i in range(amount - 1) if counts[i] < limit]
        mass, remaining = sum([loads[i] for i in free]), rest
        for i in free:
            extra = min(limit - counts[i], max(1, remaining * loads[i] // mass), rest)
            counts[i] = counts[i] + extra
            rest = rest - extra
    return np.array([limit] + counts)


def ragged_sizes(key, amount, total, limit, skew):
    if amount == 2:
        one = jax.random.randint(key, (), max(1, total - limit), min(limit, total - 1) + 1)
        return jnp.stack([one, total - one])
    lengths = jnp.asarray(split_up(amount, total, limit, skew), jnp.int32)
    pairs = (amount - 1) // 2
    source_of, taker = lengths[1:1 + 2 * pairs:2], lengths[2:2 + 2 * pairs:2]
    margin = jnp.minimum(source_of - 1, limit - taker)
    shifted = jax.random.randint(jax.random.fold_in(key, 1), (pairs,), 0, 1 << 20) % (margin + 1)
    lengths = lengths.at[1:1 + 2 * pairs:2].set(source_of - shifted).at[2:2 + 2 * pairs:2].set(taker + shifted)
    return lengths[jax.random.permutation(jax.random.fold_in(key, 2), amount)]


def gaussian(key, extent, width, reach, cuts=(), kind=jnp.bfloat16):
    values = jax.random.normal(key, extent, jnp.float32) * width
    if len(cuts) > 0:
        values = level_of(key, extent, cuts, -0.22, 0.18) * values
    return jnp.clip(values, min=-reach, max=reach).astype(kind)


def setup_inputs(seed: int = 0) -> dict:
    arg_keys = jax.random.split(jax.random.key(seed), 6)
    return {
        "q_latent": gaussian(arg_keys[0], (LAYERS, TOKENS, D_Q), 1.0, 6.0, ((0, 4), (1, 4))),
        "kv_latent": gaussian(arg_keys[1], (LAYERS, TOKENS, D_KV + ROPE), 1.0, 6.0, ((0, 4), (1, 4))),
        "segment_ids": jnp.searchsorted(jnp.cumsum(ragged_sizes(arg_keys[2], max(4, TOKENS // 64), TOKENS, min(512, TOKENS // 2), 1)), jnp.arange(TOKENS), side="right").astype(jnp.int32),
        "q_weight": draw_q_weight(jax.random.fold_in(arg_keys[5], 71), 0),
        "k_weight": gaussian(arg_keys[4], (LAYERS, D_KV, HEADS * NOPE), D_KV ** -0.5, 0.25, ((0, 4), (2, 2))),
    }


clip_threshold = 100.0
rope_base = 50000.0

def rotate(values, positions):
    half_width = values.shape[-1] // 2
    frequency = rope_base ** (-jnp.arange(half_width, dtype=jnp.float32) / half_width)
    angles = positions[:, None].astype(jnp.float32) * frequency[None, :]
    cosine = jnp.cos(angles)[:, None, :]
    sine_part = jnp.sin(angles)[:, None, :]
    lower_half = values[..., :half_width]
    upper_half = values[..., half_width:]
    return jnp.concatenate([lower_half * cosine - upper_half * sine_part, upper_half * cosine + lower_half * sine_part], -1)

def sequence_maxima(q_full, kv_rows, segments, w_key):
    length = kv_rows.shape[0]
    heads_here = w_key.shape[1] // NOPE
    q_full = q_full.reshape(length, heads_here, NOPE + ROPE)
    positions = jnp.arange(length, dtype=jnp.int32)
    queries = jnp.concatenate([q_full[..., :NOPE], rotate(q_full[..., NOPE:], positions)], -1).astype(jnp.bfloat16)
    key_nope = jnp.dot(kv_rows[:, :D_KV], w_key, preferred_element_type=jnp.float32).astype(jnp.bfloat16)
    key_nope = key_nope.reshape(length, heads_here, NOPE)
    key_rope = jnp.broadcast_to(kv_rows[:, None, D_KV:], (length, heads_here, ROPE))
    keys_all = jnp.concatenate([key_nope, key_rope], -1)
    logits = jnp.einsum('shd,thd->hst', queries.astype(jnp.float32), keys_all.astype(jnp.float32))
    logits = logits * (NOPE + ROPE) ** (-0.5)
    allowed = (segments[:, None] == segments[None, :]) & (positions[None, :] <= positions[:, None])
    return lax.optimization_barrier(jnp.max(jnp.where(allowed[None], logits, -1e+30), axis=(1, 2)))

def scale_weights(own_max, q_weight, k_weight):
    factor = clip_threshold / jnp.maximum(own_max, clip_threshold)
    square_root = jnp.sqrt(factor)
    layers_here, heads_here = own_max.shape
    column_scale = jnp.concatenate([jnp.broadcast_to(square_root[..., None], (layers_here, heads_here, NOPE)), jnp.broadcast_to(factor[..., None], (layers_here, heads_here, ROPE))], -1)
    rows_q = q_weight.shape[1]
    scaled_q = (q_weight.astype(jnp.float32).reshape(layers_here, rows_q, heads_here, NOPE + ROPE) * column_scale[:, None]).reshape(q_weight.shape).astype(jnp.bfloat16)
    scaled_k = (k_weight.astype(jnp.float32).reshape(layers_here, D_KV, heads_here, NOPE) * square_root[:, None, :, None]).reshape(k_weight.shape).astype(jnp.bfloat16)
    return (scaled_q, scaled_k)

def reference(q_latent, kv_latent, segment_ids, q_weight, k_weight):
    seg_rows = segment_ids.reshape(N_DP, SEQ)
    layer_rows = []
    for layer_idx in range(LAYERS):
        w_query = q_weight[layer_idx]
        w_key = k_weight[layer_idx]

        def one_sequence(inputs):
            latent_q, kv_rows, segments = inputs
            q_full = jnp.dot(latent_q, w_query, preferred_element_type=jnp.float32)
            return sequence_maxima(q_full, kv_rows, segments, w_key)
        per_sequence = lax.map(one_sequence, (q_latent[layer_idx].reshape(N_DP, SEQ, D_Q), kv_latent[layer_idx].reshape(N_DP, SEQ, D_KV + ROPE), seg_rows))
        layer_rows.append(lax.optimization_barrier(jnp.max(per_sequence, axis=0)))
    max_table = jnp.stack(layer_rows)
    scaled_q, scaled_k = scale_weights(max_table, q_weight, k_weight)
    return (max_table / clip_threshold, scaled_q, scaled_k)
```

```python
import functools
import jax
import jax.numpy as jnp
import numpy as np
from jax import lax
from jax.experimental import pallas as pl
from jax.experimental.pallas import tpu as pltpu
from jax.sharding import PartitionSpec as P

D_KV = 512
NOPE = 128
ROPE = 64
HEAD = NOPE + ROPE
LANES = 128
NEG = -1e30
VMEM_MIB = 44
MESH = pl.DeviceIdType.MESH

clip_threshold = 100.0
rope_base = 50000.0


def rotate(values, positions):
    half_width = values.shape[-1] // 2
    frequency = rope_base ** (-jnp.arange(half_width, dtype=jnp.float32) / half_width)
    angles = positions[:, None].astype(jnp.float32) * frequency[None, :]
    cosine = jnp.cos(angles)[:, None, :]
    sine_part = jnp.sin(angles)[:, None, :]
    lower_half = values[..., :half_width]
    upper_half = values[..., half_width:]
    return jnp.concatenate(
        [
            lower_half * cosine - upper_half * sine_part,
            upper_half * cosine + lower_half * sine_part,
        ],
        -1,
    )


def sequence_maxima(q_full, kv_rows, segments, w_key):
    length = kv_rows.shape[0]
    heads_here = w_key.shape[1] // NOPE
    q_full = q_full.reshape(length, heads_here, HEAD)
    positions = jnp.arange(length, dtype=jnp.int32)
    queries = jnp.concatenate(
        [q_full[..., :NOPE], rotate(q_full[..., NOPE:], positions)], -1
    ).astype(jnp.bfloat16)
    key_nope = jnp.dot(kv_rows[:, :D_KV], w_key, preferred_element_type=jnp.float32).astype(
        jnp.bfloat16
    )
    key_nope = key_nope.reshape(length, heads_here, NOPE)
    key_rope = jnp.broadcast_to(kv_rows[:, None, D_KV:], (length, heads_here, ROPE))
    keys_all = jnp.concatenate([key_nope, key_rope], -1)
    logits = jnp.einsum("shd,thd->hst", queries, keys_all, preferred_element_type=jnp.float32)
    logits = logits * HEAD ** (-0.5)
    allowed = (segments[:, None] == segments[None, :]) & (positions[None, :] <= positions[:, None])
    return jnp.max(jnp.where(allowed[None], logits, NEG), axis=(1, 2))


def scale_weights(own_max, q_weight, k_weight):
    factor = clip_threshold / jnp.maximum(own_max, clip_threshold)
    square_root = jnp.sqrt(factor)
    layers, heads = own_max.shape
    q_columns = jnp.concatenate(
        [
            jnp.broadcast_to(square_root[..., None], (layers, heads, NOPE)),
            jnp.broadcast_to(factor[..., None], (layers, heads, ROPE)),
        ],
        -1,
    ).reshape(layers, 1, heads * HEAD)
    k_columns = jnp.broadcast_to(square_root[..., None], (layers, heads, NOPE)).reshape(
        layers, 1, heads * NOPE
    )
    scaled_q = (q_weight.astype(jnp.float32) * q_columns).astype(jnp.bfloat16)
    scaled_k = (k_weight.astype(jnp.float32) * k_columns).astype(jnp.bfloat16)
    return scaled_q, scaled_k


def gathered_maxima(q_latent, kv_latent, segment_ids, q_weight, k_weight):
    q_full = jnp.dot(
        q_latent[0],
        lax.all_gather(q_weight[0], "dp", axis=0, tiled=True),
        preferred_element_type=jnp.float32,
    )
    own_max = sequence_maxima(q_full, kv_latent[0], segment_ids, k_weight[0])[None]
    layer_max = lax.pmax(own_max, "dp")
    return layer_max, lax.all_gather(layer_max, "section", axis=0, tiled=True)


def rope_tables(length):
    half = ROPE // 2
    frequency = np.float32(rope_base) ** (-np.arange(half, dtype=np.float32) / np.float32(half))
    angles = np.arange(length, dtype=np.float32)[:, None] * frequency[None, :].astype(np.float32)
    cosine, sine = np.cos(angles), np.sin(angles)
    zero = np.zeros_like(cosine)
    rest = np.zeros((length, ROPE), np.float32)
    low = [
        np.concatenate([cosine, cosine, rest + 1], 1),
        np.concatenate([-sine, zero, rest], 1),
        np.concatenate([zero, sine, rest], 1),
    ]
    high = [np.roll(t, ROPE, 1) for t in low]
    return np.stack(low + high).astype(np.float32)


def maxima_kernel(
    n_sec, x_hbm, kv_hbm, seg_hbm, q_hbm, k_hbm, tab_hbm, out_ref,
    lat, kvt, seg, wq, wk, keys, bias, macc, tbuf, qacc, tab_ref, tab_sem,
    lat_recv, lat_send, seg_recv, seg_send, w_recv, w_send, k_recv, k_send, t_recv, t_send,
):
    n_seq, length, _ = lat.shape
    rows = q_hbm.shape[0]
    n_pair, d_q, pair = wq.shape
    group_q, group_k = n_pair * pair, wk.shape[1]
    part = length // 2
    last = n_pair - 1
    third = rows // 3
    pieces = [(p, 0, rows) for p in range(last)] + [(last, i * third, third) for i in range(3)]

    z, sec, y = lax.axis_index("dp"), lax.axis_index("section"), lax.axis_index("head")
    c = lax.rem(sec, 2)
    half, z_low = z // 2, lax.rem(z, 2)
    base = sec - c
    primary = c == half
    core_peer = {"section": base + 1 - c}
    y_peer = {"head": 1 - y}
    z_peer = {"dp": 2 * half + 1 - z_low}
    entry = jnp.where(half == 0, 1, 2)
    me = z * n_sec + sec

    barrier = pltpu.get_barrier_semaphore()
    for step in range(1, n_seq * n_sec):
        other = lax.rem(me + step, n_seq * n_sec)
        pl.semaphore_signal(
            barrier, inc=1, device_id={"dp": other // n_sec, "section": lax.rem(other, n_sec)},
            device_id_type=MESH,
        )
    pl.semaphore_signal(barrier, inc=1, device_id=y_peer, device_id_type=MESH)

    def local(src, dst, sem):
        return pltpu.make_async_copy(src, dst, sem)

    def ready(dst, sem):
        pltpu.make_async_copy(dst, dst, sem).wait()

    def remote(src, dst, send, recv, where):
        return pltpu.make_async_remote_copy(
            src_ref=src, dst_ref=dst, send_sem=send, recv_sem=recv,
            device_id=where, device_id_type=MESH,
        )

    def slots(seq, h):
        at = pl.ds(pl.multiple_of(h * part, part), part)
        return lat.at[seq, at, :], kvt.at[seq, :, at]

    def own(h):
        at = pl.ds(pl.multiple_of(h * part, part), part)
        return x_hbm.at[at, :], kv_hbm.at[:, at]

    def send(sources, seq, h, at, where, do):
        for i, (src, dst) in enumerate(zip(sources, slots(seq, h))):
            getattr(
                remote(src, dst, lat_send.at[at, i], lat_recv.at[seq, h, i], where), do
            )()

    def ready_half(seq, h):
        for i, dst in enumerate(slots(seq, h)):
            ready(dst, lat_recv.at[seq, h, i])

    own_group = 2 * z_low + c
    peer_group = 2 * z_low + 1 - c

    def group_columns(g):
        return k_hbm.at[:, pl.ds(pl.multiple_of(g * group_k, group_k), group_k)]

    def seg_copy(step):
        return remote(
            seg_hbm, seg.at[z], seg_send.at[step], seg_recv.at[z],
            {"dp": lax.rem(z + step, n_seq)},
        )

    def own_sends(do):
        for step in range(1, n_seq):
            getattr(seg_copy(step), do)()

        @pl.when(jnp.logical_not(primary))
        def _():
            send(own(y), z, y, 0, {"dp": 3 - entry}, do)

        @pl.when(primary)
        def _():
            send(own(y), z, y, 0, z_peer, do)
            for h in range(2):
                send(own(h), z, h, 1 + h, core_peer, do)
            k_peer = remote(group_columns(peer_group), wk, k_send, k_recv, core_peer)
            getattr(k_peer, do)()

    def columns(piece, j, act):
        p, first_row, count = pieces[piece]
        if p < last:
            turn_to = lax.rem(j + 2 * z_low, 4)
        else:
            turn_to = 2 * (c if j < 2 else 1 - c) + lax.rem(j + z_low, 2)
        z_to, c_to = 2 * c + turn_to // 2, lax.rem(turn_to, 2)
        offset = pl.multiple_of(turn_to * group_q + p * pair, LANES)
        src = q_hbm.at[pl.ds(first_row, count), pl.ds(offset, pair)]
        dst = wq.at[p, pl.ds(pl.multiple_of(z * rows + first_row, third), count), :]
        mine = (z_to == z) & (c_to == c)
        there = {"dp": z_to, "section": base + c_to}
        if act == "start":
            @pl.when(mine)
            def _():
                local(src, dst, w_recv.at[piece, z]).start()

        @pl.when(jnp.logical_not(mine))
        def _():
            getattr(remote(src, dst, w_send.at[piece, j], w_recv.at[piece, z], there), act)()

    def send_columns(p):
        for j in range(4):
            for piece in range(len(pieces)):
                if pieces[piece][0] == p:
                    columns(piece, j, "start")

    def wait_rows(piece, source):
        p, first_row, count = pieces[piece]
        at = pl.ds(pl.multiple_of(source * rows + first_row, third), count)
        ready(wq.at[p, at, :], w_recv.at[piece, source])

    pl.semaphore_wait(barrier, n_seq * n_sec)

    own_sends("start")
    local(seg_hbm, seg.at[z], seg_recv.at[z]).start()
    local(tab_hbm, tab_ref, tab_sem).start()

    @pl.when(primary)
    def _():
        for h in range(2):
            for i, (src, dst) in enumerate(zip(own(h), slots(z, h))):
                local(src, dst, lat_recv.at[z, h, i]).start()
        local(group_columns(own_group), wk, k_recv).start()

    send_columns(0)
    send_columns(1)

    others = [2 * half + 1 - z_low, jnp.where(half == 0, 2, 1), jnp.where(half == 0, 3, 0)]
    at_entry = z == entry

    def relay_first(i, seq, do):
        if i > 0:
            @pl.when(at_entry)
            def _():
                send(slots(seq, y), seq, y, 6 + 4 * i, z_peer, do)
        send(slots(seq, y), seq, y, 5 + 4 * i, y_peer, do)
        send(slots(seq, y), seq, y, 3 + 4 * i, core_peer, do)

    def relay_second(i, seq, do):
        send(slots(seq, 1 - y), seq, 1 - y, 4 + 4 * i, core_peer, do)

    @pl.when(primary)
    def _():
        for i, seq in enumerate(others):
            ready_half(seq, y)
            relay_first(i, seq, "start")
        for i, seq in enumerate(others):
            ready_half(seq, 1 - y)
            relay_second(i, seq, "start")
        for h in range(2):
            ready_half(z, h)

    send_columns(2)
    send_columns(3)

    @pl.when(jnp.logical_not(primary))
    def _():
        for seq in range(n_seq):
            for h in range(2):
                ready_half(seq, h)

    ready(wk, k_recv)
    ready(tab_ref, tab_sem)
    for seq in range(n_seq):
        ready(seg.at[seq], seg_recv.at[seq])

    macc[...] = jnp.full(macc.shape, NEG, jnp.float32)

    def seq_keys(s, carry):
        seg_row = seg[s].astype(jnp.float32)
        seg_col = jnp.broadcast_to(seg_row, (LANES, length)).T[:, :1]
        row = lax.broadcasted_iota(jnp.int32, (length, length), 0)
        col = lax.broadcasted_iota(jnp.int32, (length, length), 1)
        bias[s] = jnp.where((seg_col == seg_row) & (col <= row), 0.0, NEG)
        rope = kvt[s, D_KV:, :]
        none = jnp.zeros((ROPE, length), jnp.bfloat16)
        for p in range(n_pair):
            k2 = lax.dot_general(
                wk[:, p * 2 * NOPE:(p + 1) * 2 * NOPE], kvt[s, :D_KV, :],
                (((0,), (0,)), ((), ())), preferred_element_type=jnp.float32,
            ).astype(jnp.bfloat16)
            keys[s, p, 0, :NOPE, :] = k2[:NOPE]
            keys[s, p, 0, NOPE:HEAD, :] = rope
            keys[s, p, 0, HEAD:, :] = none
            keys[s, p, 1, :ROPE, :] = none
            keys[s, p, 1, ROPE:HEAD, :] = k2[NOPE:]
            keys[s, p, 1, HEAD:, :] = rope
        return carry

    lax.fori_loop(0, n_seq, seq_keys, 0)

    def turn(values, at):
        return (
            values * tab_ref[at]
            + pltpu.roll(values, LANES - ROPE // 2, 1) * tab_ref[at + 1]
            + pltpu.roll(values, ROPE // 2, 1) * tab_ref[at + 2]
        ).astype(jnp.bfloat16)

    def pair_maxima(p, s, q2):
        first = q2[:, :NOPE].astype(jnp.bfloat16)
        middle = turn(q2[:, NOPE:2 * NOPE], 0)
        final = turn(q2[:, 2 * NOPE:], 3)
        for e, tiles in enumerate(((first, middle), (middle, final))):
            queries = jnp.concatenate(tiles, 1)
            for block in range(2):
                lo, hi = block * part, (block + 1) * part
                logits = jnp.dot(
                    queries[lo:hi], keys[s, p, e, :, :hi], preferred_element_type=jnp.float32
                ) + bias[s, lo:hi, :hi]
                top = jnp.max(logits.reshape(part // 8, 8, hi), axis=0)
                macc[2 * p + e, :, :hi] = jnp.maximum(macc[2 * p + e, :, :hi], top)

    def pair_logits(p, carry):
        for source in range(n_seq):
            at = pl.ds(source * rows, rows)
            ready(wq.at[p, at, :], w_recv.at[p, source])

        def one(s, inner):
            pair_maxima(p, s, jnp.dot(lat[s], wq[p], preferred_element_type=jnp.float32))
            return inner

        return lax.fori_loop(0, n_seq, one, carry)

    lax.fori_loop(0, last, pair_logits, 0)

    def partial(s, start, count):
        at = pl.ds(pl.multiple_of(start, third), count)
        return jnp.dot(lat[s, :, at], wq[last, at, :], preferred_element_type=jnp.float32)

    near_rows = half * 2 * rows
    far_rows = (2 * (1 - half) + c) * rows
    final_source = 2 * (1 - half) + 1 - c
    final_rows = final_source * rows

    def from_near(s, carry):
        qacc[s] = partial(s, near_rows, 2 * rows)
        return carry

    def from_far(s, carry):
        qacc[s] = qacc[s] + partial(s, far_rows, rows)
        return carry

    def from_final(s, carry):
        qacc[s] = qacc[s] + partial(s, final_rows, 2 * third)
        return carry

    def finish(s, carry):
        pair_maxima(last, s, qacc[s] + partial(s, final_rows + 2 * third, third))
        return carry

    for z_of in range(2):
        for piece in range(last, len(pieces)):
            wait_rows(piece, 2 * half + z_of)
    lax.fori_loop(0, n_seq, from_near, 0)
    for piece in range(last, len(pieces)):
        wait_rows(piece, 2 * (1 - half) + c)
    lax.fori_loop(0, n_seq, from_far, 0)
    for piece in range(last, last + 2):
        wait_rows(piece, final_source)
    lax.fori_loop(0, n_seq, from_final, 0)
    wait_rows(last + 2, final_source)
    lax.fori_loop(0, n_seq, finish, 0)

    top = jnp.max(jnp.max(macc[...], axis=1), axis=1, keepdims=True) * HEAD ** (-0.5)
    tile = jnp.broadcast_to(top, tbuf.shape)
    tbuf[...] = tile
    out_ref[me] = tile

    def table_copy(step):
        other = lax.rem(me + step, n_seq * n_sec)
        return remote(
            tbuf, out_ref.at[me], t_send.at[step], t_recv.at[me],
            {"dp": other // n_sec, "section": lax.rem(other, n_sec)},
        )

    for step in range(1, n_seq * n_sec):
        table_copy(step).start()
    for piece in range(len(pieces)):
        for j in range(4):
            columns(piece, j, "wait_send")
    own_sends("wait_send")

    @pl.when(primary)
    def _():
        for i, seq in enumerate(others):
            relay_first(i, seq, "wait_send")
            relay_second(i, seq, "wait_send")

    for step in range(1, n_seq * n_sec):
        source = lax.rem(me + step, n_seq * n_sec)
        ready(out_ref.at[source], t_recv.at[source])
    for step in range(1, n_seq * n_sec):
        table_copy(step).wait_send()


def scale_kernel(
    n_sec, table, q_ref, k_ref, ratio_ref, q_out, k_out, q_buf, k_buf, q_row, k_row, q_sem, k_sem
):
    group = table.shape[1]
    n_group, n_pair = q_ref.shape[1] // (group * HEAD), group // 2
    n_chunk = q_sem.shape[0]
    sec = lax.axis_index("section")
    low = lax.broadcasted_iota(jnp.int32, (1, LANES), 1) < ROPE

    def slot(layer, number):
        z_of = 2 * (layer % 2) + number // 2
        return z_of * n_sec + 2 * (layer // 2) + number % 2

    for g in range(n_group):
        factor = clip_threshold / jnp.maximum(table[slot(sec, g)], clip_threshold)
        root = jnp.sqrt(factor)
        for p in range(n_pair):
            f_a, f_b = factor[2 * p:2 * p + 1], factor[2 * p + 1:2 * p + 2]
            r_a, r_b = root[2 * p:2 * p + 1], root[2 * p + 1:2 * p + 2]
            number = g * n_pair + p
            scales = (r_a, jnp.where(low, f_a, r_b), jnp.where(low, r_b, f_b))
            for i, scale in enumerate(scales):
                q_row[:, pl.ds((3 * number + i) * LANES, LANES)] = scale
            for i, scale in enumerate((r_a, r_b)):
                k_row[:, pl.ds((2 * number + i) * LANES, LANES)] = scale

    def block(source, target, sem, i):
        count = source.shape[0] // n_chunk
        at = pl.ds(pl.multiple_of(i * count, count), count)
        return at, pltpu.make_async_copy(source.at[at, :], target.at[at, :], sem.at[i])

    def one_chunk(i, carry):
        for source, row, buf, target, sem in (
            (q_ref, q_row, q_buf, q_out, q_sem), (k_ref, k_row, k_buf, k_out, k_sem),
        ):
            at, copy = block(buf, target, sem, i)
            for tile in range(source.shape[1] // LANES):
                lanes = pl.ds(tile * LANES, LANES)
                values = source[at, lanes].astype(jnp.float32) * row[:, lanes]
                buf[at, lanes] = values.astype(jnp.bfloat16)
            copy.start()
        return carry

    lax.fori_loop(0, n_chunk, one_chunk, 0)

    lane = lax.broadcasted_iota(jnp.int32, (group, LANES), 1)
    place = lax.broadcasted_iota(jnp.int32, (group, LANES), 0)
    for layer in range(ratio_ref.shape[0]):
        line = jnp.zeros((1, LANES), jnp.float32)
        for number in range(n_group):
            values = table[slot(layer, number)]
            here = lane == number * group + place
            line = line + jnp.sum(jnp.where(here, values, 0.0), axis=0, keepdims=True)
        ratio_ref[layer:layer + 1, :] = line[:, :ratio_ref.shape[1]] / clip_threshold

    for i in range(n_chunk):
        block(q_buf, q_out, q_sem, i)[1].wait()
        block(k_buf, k_out, k_sem, i)[1].wait()


def exchanged(sizes, q_latent, kv_latent, segment_ids, q_weight, k_weight):
    n_dp, n_sec = sizes
    _, length, d_q = q_latent.shape
    rows = q_weight.shape[1]
    heads = k_weight.shape[2] // NOPE
    group = heads // n_dp
    n_pair = group // 2
    bf16, dma = jnp.bfloat16, pltpu.SemaphoreType.DMA
    n_all = n_dp * n_sec
    table = pl.pallas_call(
        functools.partial(maxima_kernel, n_sec),
        out_shape=jax.ShapeDtypeStruct((n_all, group, LANES), jnp.float32),
        in_specs=[pl.BlockSpec(memory_space=pltpu.HBM)] * 6,
        out_specs=pl.BlockSpec(memory_space=pltpu.VMEM),
        scratch_shapes=[
            pltpu.VMEM((n_dp, length, d_q), bf16),
            pltpu.VMEM((n_dp, D_KV + ROPE, length), bf16),
            pltpu.VMEM((n_dp, 1, length), jnp.int32),
            pltpu.VMEM((n_pair, d_q, 2 * HEAD), bf16),
            pltpu.VMEM((D_KV, group * NOPE), bf16),
            pltpu.VMEM((n_dp, n_pair, 2, 2 * NOPE, length), bf16),
            pltpu.VMEM((n_dp, length, length), jnp.float32),
            pltpu.VMEM((group, 8, length), jnp.float32),
            pltpu.VMEM((group, LANES), jnp.float32),
            pltpu.VMEM((n_dp, length, 2 * HEAD), jnp.float32),
            pltpu.VMEM((6, length, LANES), jnp.float32),
            dma,
            dma((n_dp, 2, 2)),
            dma((15, 2)),
            dma((n_dp,)),
            dma((n_dp,)),
            dma((n_pair + 2, n_dp)),
            dma((n_pair + 2, 4)),
            dma,
            dma,
            dma((n_all,)),
            dma((n_all,)),
        ],
        compiler_params=pltpu.CompilerParams(
            collective_id=0, has_side_effects=True, vmem_limit_bytes=VMEM_MIB * 1024 * 1024
        ),
        cost_estimate=pl.CostEstimate(
            flops=2 * n_dp * length * group * (HEAD * (d_q + length) + NOPE * D_KV),
            bytes_accessed=2 * rows * heads * HEAD, transcendentals=0,
        ),
        name="maxima",
    )(
        *[
            pltpu.with_memory_space_constraint(a, pltpu.HBM)
            for a in (
                q_latent[0], kv_latent[0].T, segment_ids.reshape(1, length), q_weight[0],
                k_weight[0], jnp.asarray(rope_tables(length)),
            )
        ],
    )
    ratio, scaled_q, scaled_k = pl.pallas_call(
        functools.partial(scale_kernel, n_sec),
        out_shape=(
            jax.ShapeDtypeStruct((n_sec, heads), jnp.float32),
            jax.ShapeDtypeStruct(q_weight.shape[1:], bf16),
            jax.ShapeDtypeStruct(k_weight.shape[1:], bf16),
        ),
        in_specs=[pl.BlockSpec(memory_space=pltpu.VMEM)] * 3,
        out_specs=[pl.BlockSpec(memory_space=pltpu.VMEM)]
        + [pl.BlockSpec(memory_space=pltpu.HBM)] * 2,
        scratch_shapes=[
            pltpu.VMEM(q_weight.shape[1:], bf16),
            pltpu.VMEM(k_weight.shape[1:], bf16),
            pltpu.VMEM((1, q_weight.shape[2]), jnp.float32),
            pltpu.VMEM((1, k_weight.shape[2]), jnp.float32),
            dma((8,)),
            dma((8,)),
        ],
        compiler_params=pltpu.CompilerParams(vmem_limit_bytes=24 * 1024 * 1024),
        cost_estimate=pl.CostEstimate(
            flops=rows * heads * HEAD, bytes_accessed=8 * rows * heads * HEAD, transcendentals=0
        ),
        name="scale",
    )(table, q_weight[0], k_weight[0])
    return ratio, scaled_q[None], scaled_k[None]


def per_device(sizes, q_latent, kv_latent, segment_ids, q_weight, k_weight):
    n_dp, n_sec, n_head = sizes
    heads = k_weight.shape[2] // NOPE
    length = q_latent.shape[1]
    exchange = (
        n_dp == 4 and n_sec % 2 == 0 and q_weight.shape[1] % 384 == 0 and n_head == 2 and heads == 8 * n_dp
        and length % 512 == 0 and q_latent.shape[0] == 1
    )
    args = (q_latent, kv_latent, segment_ids, q_weight, k_weight)
    if exchange:
        return exchanged((n_dp, n_sec), *args)
    own, max_table = gathered_maxima(*args)
    scaled_q, scaled_k = scale_weights(own, q_weight, k_weight)
    return max_table / clip_threshold, scaled_q, scaled_k


def solution(mesh):
    sizes = tuple(mesh.shape[axis] for axis in ("dp", "section", "head"))
    return jax.shard_map(
        functools.partial(per_device, sizes),
        mesh=mesh,
        in_specs=(
            P("section", "dp", None),
            P("section", "dp", None),
            P("dp"),
            P("section", "dp", "head"),
            P("section", None, "head"),
        ),
        out_specs=(P(None, "head"), P("section", "dp", "head"), P("section", None, "head")),
        check_vma=False,
    )
```

```python
import functools
import jax
import jax.numpy as jnp
import numpy as np
from jax import lax
from jax.experimental import pallas as pl
from jax.experimental.pallas import tpu as pltpu
from jax.sharding import PartitionSpec as P

D_KV = 512
NOPE = 128
ROPE = 64
HEAD = NOPE + ROPE
LANES = 128
NEG = -1e30
VMEM_MIB = 44
MESH = pl.DeviceIdType.MESH

clip_threshold = 100.0
rope_base = 50000.0


def rotate(values, positions):
    half_width = values.shape[-1] // 2
    frequency = rope_base ** (-jnp.arange(half_width, dtype=jnp.float32) / half_width)
    angles = positions[:, None].astype(jnp.float32) * frequency[None, :]
    cosine = jnp.cos(angles)[:, None, :]
    sine_part = jnp.sin(angles)[:, None, :]
    lower_half = values[..., :half_width]
    upper_half = values[..., half_width:]
    return jnp.concatenate(
        [
            lower_half * cosine - upper_half * sine_part,
            upper_half * cosine + lower_half * sine_part,
        ],
        -1,
    )


def sequence_maxima(q_full, kv_rows, segments, w_key):
    length = kv_rows.shape[0]
    heads_here = w_key.shape[1] // NOPE
    q_full = q_full.reshape(length, heads_here, HEAD)
    positions = jnp.arange(length, dtype=jnp.int32)
    queries = jnp.concatenate(
        [q_full[..., :NOPE], rotate(q_full[..., NOPE:], positions)], -1
    ).astype(jnp.bfloat16)
    key_nope = jnp.dot(kv_rows[:, :D_KV], w_key, preferred_element_type=jnp.float32).astype(
        jnp.bfloat16
    )
    key_nope = key_nope.reshape(length, heads_here, NOPE)
    key_rope = jnp.broadcast_to(kv_rows[:, None, D_KV:], (length, heads_here, ROPE))
    keys_all = jnp.concatenate([key_nope, key_rope], -1)
    logits = jnp.einsum("shd,thd->hst", queries, keys_all, preferred_element_type=jnp.float32)
    logits = logits * HEAD ** (-0.5)
    allowed = (segments[:, None] == segments[None, :]) & (positions[None, :] <= positions[:, None])
    return jnp.max(jnp.where(allowed[None], logits, NEG), axis=(1, 2))


def scale_weights(own_max, q_weight, k_weight):
    factor = clip_threshold / jnp.maximum(own_max, clip_threshold)
    square_root = jnp.sqrt(factor)
    layers, heads = own_max.shape
    q_columns = jnp.concatenate(
        [
            jnp.broadcast_to(square_root[..., None], (layers, heads, NOPE)),
            jnp.broadcast_to(factor[..., None], (layers, heads, ROPE)),
        ],
        -1,
    ).reshape(layers, 1, heads * HEAD)
    k_columns = jnp.broadcast_to(square_root[..., None], (layers, heads, NOPE)).reshape(
        layers, 1, heads * NOPE
    )
    scaled_q = (q_weight.astype(jnp.float32) * q_columns).astype(jnp.bfloat16)
    scaled_k = (k_weight.astype(jnp.float32) * k_columns).astype(jnp.bfloat16)
    return scaled_q, scaled_k


def gathered_maxima(q_latent, kv_latent, segment_ids, q_weight, k_weight):
    q_full = jnp.dot(
        q_latent[0],
        lax.all_gather(q_weight[0], "dp", axis=0, tiled=True),
        preferred_element_type=jnp.float32,
    )
    own_max = sequence_maxima(q_full, kv_latent[0], segment_ids, k_weight[0])[None]
    layer_max = lax.pmax(own_max, "dp")
    return layer_max, lax.all_gather(layer_max, "section", axis=0, tiled=True)


def rope_tables(length):
    half = ROPE // 2
    frequency = np.float32(rope_base) ** (-np.arange(half, dtype=np.float32) / np.float32(half))
    angles = np.arange(length, dtype=np.float32)[:, None] * frequency[None, :].astype(np.float32)
    cosine, sine = np.cos(angles), np.sin(angles)
    zero = np.zeros_like(cosine)
    rest = np.zeros((length, ROPE), np.float32)
    low = [
        np.concatenate([cosine, cosine, rest + 1], 1),
        np.concatenate([-sine, zero, rest], 1),
        np.concatenate([zero, sine, rest], 1),
    ]
    high = [np.roll(t, ROPE, 1) for t in low]
    return np.stack(low + high).astype(np.float32)


def maxima_kernel(
    n_sec, x_hbm, kv_hbm, seg_hbm, q_hbm, k_hbm, tab_hbm, out_ref,
    lat, kvt, seg, wq, wk, keys, bias, macc, tbuf, qacc, mid, tab_ref, outer_sem, line_sem, side_sem, all_sem, tab_sem,
    lat_recv, lat_send, seg_recv, seg_send, w_recv, w_send, k_recv, k_send, t_recv, t_send,
):
    n_seq, length, _ = lat.shape
    rows = q_hbm.shape[0]
    n_pair, d_q, pair = wq.shape
    group_q, group_k = n_pair * pair, wk.shape[1]
    part = length // 2
    last = n_pair - 1
    third = rows // 3
    pieces = [(p, 0, rows, 0, pair) for p in range(last)]
    pieces += [
        (last, 0, rows, 0, 2 * LANES),
        (last, 0, 2 * third, 2 * LANES, LANES),
        (last, 2 * third, third, 2 * LANES, LANES),
    ]

    z, sec, y = lax.axis_index("dp"), lax.axis_index("section"), lax.axis_index("head")
    c = lax.rem(sec, 2)
    half, z_low = z // 2, lax.rem(z, 2)
    base = sec - c
    primary = c == half
    core_peer = {"section": base + 1 - c}
    y_peer = {"head": 1 - y}
    z_peer = {"dp": 2 * half + 1 - z_low}
    entry = jnp.where(half == 0, 1, 2)
    me = z * n_sec + sec

    mid_z, outer_z = 3 - z, jnp.where(half == 0, 0, 3)
    inner = z == entry
    outer = jnp.logical_not(inner)
    both_cores = [base, base + 1]
    side_peers = [{"section": lax.rem(sec + 2 * i, n_sec)} for i in range(1, n_sec // 2)]
    side_peers.append(y_peer)

    def signal(sem, where):
        pl.semaphore_signal(sem, inc=1, device_id=where, device_id_type=MESH)

    barrier = pltpu.get_barrier_semaphore()

    @pl.when(inner)
    def _():
        for there in both_cores:
            signal(barrier, {"dp": mid_z, "section": there})
        for there in both_cores:
            signal(barrier, {"dp": outer_z, "section": there})

    @pl.when(outer)
    def _():
        for where in side_peers:
            signal(barrier, where)

    def local(src, dst, sem):
        return pltpu.make_async_copy(src, dst, sem)

    def ready(dst, sem):
        pltpu.make_async_copy(dst, dst, sem).wait()

    def remote(src, dst, send, recv, where):
        return pltpu.make_async_remote_copy(
            src_ref=src, dst_ref=dst, send_sem=send, recv_sem=recv,
            device_id=where, device_id_type=MESH,
        )

    def slots(seq, h):
        at = pl.ds(pl.multiple_of(h * part, part), part)
        return lat.at[seq, at, :], kvt.at[seq, :, at]

    def own(h):
        at = pl.ds(pl.multiple_of(h * part, part), part)
        return x_hbm.at[at, :], kv_hbm.at[:, at]

    def send(sources, seq, h, at, where, do):
        for i, (src, dst) in enumerate(zip(sources, slots(seq, h))):
            getattr(
                remote(src, dst, lat_send.at[at, i], lat_recv.at[seq, h, i], where), do
            )()

    def ready_half(seq, h):
        for i, dst in enumerate(slots(seq, h)):
            ready(dst, lat_recv.at[seq, h, i])

    own_group = 2 * z_low + c
    peer_group = 2 * z_low + 1 - c

    def group_columns(g):
        return k_hbm.at[:, pl.ds(pl.multiple_of(g * group_k, group_k), group_k)]

    def seg_copy(step):
        return remote(
            seg_hbm, seg.at[z], seg_send.at[step], seg_recv.at[z],
            {"dp": lax.rem(z + step, n_seq)},
        )

    def first_send(do):
        send(own(y), z, y, 0, {"dp": 3 - entry}, do)

    def own_sends(do):
        for step in range(1, n_seq):
            getattr(seg_copy(step), do)()

        @pl.when(jnp.logical_not(primary) & (outer if do == "start" else True))
        def _():
            first_send(do)

        @pl.when(primary)
        def _():
            send(own(y), z, y, 0, z_peer, do)
            for h in range(2):
                send(own(h), z, h, 1 + h, core_peer, do)
            k_peer = remote(group_columns(peer_group), wk, k_send, k_recv, core_peer)
            getattr(k_peer, do)()

    def rows_of(piece, source):
        p, first_row, count, first_column, width = pieces[piece]
        at = pl.ds(pl.multiple_of(source * rows + first_row, third), count)
        return wq.at[p, at, pl.ds(first_column, width)]

    def columns(piece, j, act):
        p, first_row, count, first_column, width = pieces[piece]
        if p < last:
            turn_to = lax.rem(j + 2 * z_low, 4)
        else:
            turn_to = 2 * (1 - c if j < 2 else c) + j % 2
        z_to, c_to = 2 * c + turn_to // 2, lax.rem(turn_to, 2)
        offset = pl.multiple_of(turn_to * group_q + p * pair + first_column, LANES)
        src = q_hbm.at[pl.ds(first_row, count), pl.ds(offset, width)]
        dst = rows_of(piece, z)
        mine = (z_to == z) & (c_to == c)
        there = {"dp": z_to, "section": base + c_to}
        if act == "start":
            @pl.when(mine)
            def _():
                local(src, dst, w_recv.at[piece, z]).start()

        @pl.when(jnp.logical_not(mine))
        def _():
            getattr(remote(src, dst, w_send.at[piece, j], w_recv.at[piece, z], there), act)()

    def send_columns(p):
        for j in range(4):
            columns(p, j, "start")

    def send_last_columns():
        for j in range(4):
            columns(last, j, "start")
        for j in (2, 3, 0, 1):
            for piece in range(last + 1, len(pieces)):
                columns(piece, j, "start")

    def wait_rows(piece, source):
        ready(rows_of(piece, source), w_recv.at[piece, source])

    pl.semaphore_wait(barrier, jnp.where(inner, 2, 2 + len(side_peers)))

    @pl.when(inner & jnp.logical_not(primary))
    def _():
        first_send("start")

    @pl.when(outer)
    def _():
        for there in both_cores:
            signal(outer_sem, {"dp": entry, "section": there})
        pl.semaphore_wait(line_sem, 1)

    @pl.when(inner)
    def _():
        pl.semaphore_wait(outer_sem, 2)
        signal(line_sem, {"dp": mid_z})
        pl.semaphore_wait(line_sem, 1)
        signal(line_sem, {"dp": outer_z})

    own_sends("start")
    local(seg_hbm, seg.at[z], seg_recv.at[z]).start()
    local(tab_hbm, tab_ref, tab_sem).start()

    @pl.when(primary)
    def _():
        for h in range(2):
            for i, (src, dst) in enumerate(zip(own(h), slots(z, h))):
                local(src, dst, lat_recv.at[z, h, i]).start()
        local(group_columns(own_group), wk, k_recv).start()

    send_columns(0)
    send_columns(1)

    @pl.when(outer)
    def _():
        for where in side_peers:
            signal(side_sem, where)
        pl.semaphore_wait(side_sem, len(side_peers))
        signal(all_sem, {"dp": entry})

    @pl.when(inner)
    def _():
        pl.semaphore_wait(all_sem, 1)

    others = [2 * half + 1 - z_low, jnp.where(half == 0, 2, 1), jnp.where(half == 0, 3, 0)]
    at_entry = z == entry

    def relay_first(i, seq, do):
        if i > 0:
            @pl.when(at_entry)
            def _():
                send(slots(seq, y), seq, y, 6 + 4 * i, z_peer, do)
        send(slots(seq, y), seq, y, 5 + 4 * i, y_peer, do)
        send(slots(seq, y), seq, y, 3 + 4 * i, core_peer, do)

    def relay_second(i, seq, do):
        send(slots(seq, 1 - y), seq, 1 - y, 4 + 4 * i, core_peer, do)

    @pl.when(primary)
    def _():
        for i, seq in enumerate(others):
            ready_half(seq, y)
            relay_first(i, seq, "start")
        for i, seq in enumerate(others):
            ready_half(seq, 1 - y)
            relay_second(i, seq, "start")
        for h in range(2):
            ready_half(z, h)

    for p in range(2, last):
        send_columns(p)
    send_last_columns()

    @pl.when(jnp.logical_not(primary))
    def _():
        for seq in range(n_seq):
            for h in range(2):
                ready_half(seq, h)

    ready(wk, k_recv)
    ready(tab_ref, tab_sem)
    for seq in range(n_seq):
        ready(seg.at[seq], seg_recv.at[seq])

    macc[...] = jnp.full(macc.shape, NEG, jnp.float32)

    def seq_keys(s, carry):
        seg_row = seg[s].astype(jnp.float32)
        seg_col = jnp.broadcast_to(seg_row, (LANES, length)).T[:, :1]
        row = lax.broadcasted_iota(jnp.int32, (length, length), 0)
        col = lax.broadcasted_iota(jnp.int32, (length, length), 1)
        bias[s] = jnp.where((seg_col == seg_row) & (col <= row), 0.0, NEG)
        rope = kvt[s, D_KV:, :]
        none = jnp.zeros((ROPE, length), jnp.bfloat16)
        for p in range(n_pair):
            k2 = lax.dot_general(
                wk[:, p * 2 * NOPE:(p + 1) * 2 * NOPE], kvt[s, :D_KV, :],
                (((0,), (0,)), ((), ())), preferred_element_type=jnp.float32,
            ).astype(jnp.bfloat16)
            keys[s, p, 0, :NOPE, :] = k2[:NOPE]
            keys[s, p, 0, NOPE:HEAD, :] = rope
            keys[s, p, 0, HEAD:, :] = none
            keys[s, p, 1, :ROPE, :] = none
            keys[s, p, 1, ROPE:HEAD, :] = k2[NOPE:]
            keys[s, p, 1, HEAD:, :] = rope
        return carry

    lax.fori_loop(0, n_seq, seq_keys, 0)

    def turn(values, at):
        return (
            values * tab_ref[at]
            + pltpu.roll(values, LANES - ROPE // 2, 1) * tab_ref[at + 1]
            + pltpu.roll(values, ROPE // 2, 1) * tab_ref[at + 2]
        ).astype(jnp.bfloat16)

    def tops(p, e, s, tiles):
        queries = jnp.concatenate(tiles, 1)
        found = []
        for block in range(2):
            lo, hi = block * part, (block + 1) * part
            logits = jnp.dot(
                queries[lo:hi], keys[s, p, e, :, :hi], preferred_element_type=jnp.float32
            ) + bias[s, lo:hi, :hi]
            found.append(jnp.max(logits.reshape(part // 8, 8, hi), axis=0))
        return found

    def keep(p, e, found):
        for block, top in enumerate(found):
            hi = (block + 1) * part
            macc[2 * p + e, :, :hi] = jnp.maximum(macc[2 * p + e, :, :hi], top)

    def head_maxima(p, e, s, tiles):
        keep(p, e, tops(p, e, s, tiles))

    def pair_maxima(p, s, q2):
        first = q2[:, :NOPE].astype(jnp.bfloat16)
        middle = turn(q2[:, NOPE:2 * NOPE], 0)
        head_maxima(p, 0, s, (first, middle))
        head_maxima(p, 1, s, (middle, turn(q2[:, 2 * NOPE:], 3)))

    def pair_logits(p, carry):
        for source in range(n_seq):
            at = pl.ds(source * rows, rows)
            ready(wq.at[p, at, :], w_recv.at[p, source])

        def one(s, inner):
            pair_maxima(p, s, jnp.dot(lat[s], wq[p], preferred_element_type=jnp.float32))
            return inner

        return lax.fori_loop(0, n_seq, one, carry)

    lax.fori_loop(0, last, pair_logits, 0)

    def partial(s, starts, count, first_column, width):
        spans = [pl.ds(pl.multiple_of(start, third), count) for start in starts]
        tokens = [lat[s, :, at] for at in spans]
        weights = [wq[last, at, pl.ds(first_column, width)] for at in spans]
        if len(spans) > 1:
            tokens, weights = [jnp.concatenate(tokens, 1)], [jnp.concatenate(weights, 0)]
        return jnp.dot(tokens[0], weights[0], preferred_element_type=jnp.float32)

    near_sources = [2 * half, 2 * half + 1]
    far_sources = [2 * (1 - half), 2 * (1 - half) + 1]
    far_rows = [source * rows for source in far_sources]
    whole, narrow = last, slice(2 * LANES, 3 * LANES)

    def from_near(s, carry):
        qacc[s] = partial(s, [near_sources[0] * rows], 2 * rows, 0, pair)
        return carry

    def from_far(s, carry):
        q2 = qacc[s, :, :2 * LANES] + partial(s, far_rows[:1], 2 * rows, 0, 2 * LANES)
        middle = turn(q2[:, LANES:], 0)
        mid[s] = middle
        head_maxima(last, 0, s, (q2[:, :LANES].astype(jnp.bfloat16), middle))
        return carry

    def from_far_tile(s, carry):
        qacc[s, :, narrow] = qacc[s, :, narrow] + partial(
            s, far_rows, 2 * third, 2 * LANES, LANES
        )
        return carry

    def finish(s):
        starts = [start + 2 * third for start in far_rows]
        q1 = qacc[s, :, narrow] + partial(s, starts, third, 2 * LANES, LANES)
        return tops(last, 1, s, (mid[s], turn(q1, 3)))

    for source in near_sources:
        for piece in range(last, len(pieces)):
            wait_rows(piece, source)
    lax.fori_loop(0, n_seq, from_near, 0)
    for source in far_sources:
        wait_rows(whole, source)
    lax.fori_loop(0, n_seq, from_far, 0)
    for source in far_sources:
        wait_rows(last + 1, source)
    lax.fori_loop(0, n_seq, from_far_tile, 0)
    for source in far_sources:
        wait_rows(last + 2, source)
    found = [finish(s) for s in range(n_seq)]
    keep(last, 1, [functools.reduce(jnp.maximum, tops_of) for tops_of in zip(*found)])

    top = jnp.max(jnp.max(macc[...], axis=1), axis=1, keepdims=True) * HEAD ** (-0.5)
    tile = jnp.broadcast_to(top, tbuf.shape)
    tbuf[...] = tile
    out_ref[me] = tile

    def table_copy(step):
        other = lax.rem(me + step, n_seq * n_sec)
        return remote(
            tbuf, out_ref.at[me], t_send.at[step], t_recv.at[me],
            {"dp": other // n_sec, "section": lax.rem(other, n_sec)},
        )

    for step in range(1, n_seq * n_sec):
        table_copy(step).start()
    for piece in range(len(pieces)):
        for j in range(4):
            columns(piece, j, "wait_send")
    own_sends("wait_send")

    @pl.when(primary)
    def _():
        for i, seq in enumerate(others):
            relay_first(i, seq, "wait_send")
            relay_second(i, seq, "wait_send")

    for step in range(1, n_seq * n_sec):
        source = lax.rem(me + step, n_seq * n_sec)
        ready(out_ref.at[source], t_recv.at[source])
    for step in range(1, n_seq * n_sec):
        table_copy(step).wait_send()


def scale_kernel(
    n_sec, table, q_ref, k_ref, ratio_ref, q_out, k_out, q_buf, k_buf, q_row, k_row, q_sem, k_sem
):
    group = table.shape[1]
    n_group, n_pair = q_ref.shape[1] // (group * HEAD), group // 2
    n_chunk = q_sem.shape[0]
    sec = lax.axis_index("section")
    low = lax.broadcasted_iota(jnp.int32, (1, LANES), 1) < ROPE

    def slot(layer, number):
        z_of = 2 * (layer % 2) + number // 2
        return z_of * n_sec + 2 * (layer // 2) + number % 2

    for g in range(n_group):
        factor = clip_threshold / jnp.maximum(table[slot(sec, g)], clip_threshold)
        root = jnp.sqrt(factor)
        for p in range(n_pair):
            f_a, f_b = factor[2 * p:2 * p + 1], factor[2 * p + 1:2 * p + 2]
            r_a, r_b = root[2 * p:2 * p + 1], root[2 * p + 1:2 * p + 2]
            number = g * n_pair + p
            scales = (r_a, jnp.where(low, f_a, r_b), jnp.where(low, r_b, f_b))
            for i, scale in enumerate(scales):
                q_row[:, pl.ds((3 * number + i) * LANES, LANES)] = scale
            for i, scale in enumerate((r_a, r_b)):
                k_row[:, pl.ds((2 * number + i) * LANES, LANES)] = scale

    def block(source, target, sem, i):
        count = source.shape[0] // n_chunk
        at = pl.ds(pl.multiple_of(i * count, count), count)
        return at, pltpu.make_async_copy(source.at[at, :], target.at[at, :], sem.at[i])

    def one_chunk(i, carry):
        for source, row, buf, target, sem in (
            (q_ref, q_row, q_buf, q_out, q_sem), (k_ref, k_row, k_buf, k_out, k_sem),
        ):
            at, copy = block(buf, target, sem, i)
            for tile in range(source.shape[1] // LANES):
                lanes = pl.ds(tile * LANES, LANES)
                values = source[at, lanes].astype(jnp.float32) * row[:, lanes]
                buf[at, lanes] = values.astype(jnp.bfloat16)
            copy.start()
        return carry

    lax.fori_loop(0, n_chunk, one_chunk, 0)

    lane = lax.broadcasted_iota(jnp.int32, (group, LANES), 1)
    place = lax.broadcasted_iota(jnp.int32, (group, LANES), 0)
    for layer in range(ratio_ref.shape[0]):
        line = jnp.zeros((1, LANES), jnp.float32)
        for number in range(n_group):
            values = table[slot(layer, number)]
            here = lane == number * group + place
            line = line + jnp.sum(jnp.where(here, values, 0.0), axis=0, keepdims=True)
        ratio_ref[layer:layer + 1, :] = line[:, :ratio_ref.shape[1]] / clip_threshold

    for i in range(n_chunk):
        block(q_buf, q_out, q_sem, i)[1].wait()
        block(k_buf, k_out, k_sem, i)[1].wait()


def exchanged(sizes, q_latent, kv_latent, segment_ids, q_weight, k_weight):
    n_dp, n_sec = sizes
    _, length, d_q = q_latent.shape
    rows = q_weight.shape[1]
    heads = k_weight.shape[2] // NOPE
    group = heads // n_dp
    n_pair = group // 2
    bf16, dma = jnp.bfloat16, pltpu.SemaphoreType.DMA
    n_all = n_dp * n_sec
    table = pl.pallas_call(
        functools.partial(maxima_kernel, n_sec),
        out_shape=jax.ShapeDtypeStruct((n_all, group, LANES), jnp.float32),
        in_specs=[pl.BlockSpec(memory_space=pltpu.HBM)] * 6,
        out_specs=pl.BlockSpec(memory_space=pltpu.VMEM),
        scratch_shapes=[
            pltpu.VMEM((n_dp, length, d_q), bf16),
            pltpu.VMEM((n_dp, D_KV + ROPE, length), bf16),
            pltpu.VMEM((n_dp, 1, length), jnp.int32),
            pltpu.VMEM((n_pair, d_q, 2 * HEAD), bf16),
            pltpu.VMEM((D_KV, group * NOPE), bf16),
            pltpu.VMEM((n_dp, n_pair, 2, 2 * NOPE, length), bf16),
            pltpu.VMEM((n_dp, length, length), jnp.float32),
            pltpu.VMEM((group, 8, length), jnp.float32),
            pltpu.VMEM((group, LANES), jnp.float32),
            pltpu.VMEM((n_dp, length, 2 * HEAD), jnp.float32),
            pltpu.VMEM((n_dp, length, LANES), bf16),
            pltpu.VMEM((6, length, LANES), jnp.float32),
            *[pltpu.SemaphoreType.REGULAR] * 4,
            dma,
            dma((n_dp, 2, 2)),
            dma((15, 2)),
            dma((n_dp,)),
            dma((n_dp,)),
            dma((n_pair + 2, n_dp)),
            dma((n_pair + 2, 4)),
            dma,
            dma,
            dma((n_all,)),
            dma((n_all,)),
        ],
        compiler_params=pltpu.CompilerParams(
            collective_id=0, has_side_effects=True, vmem_limit_bytes=VMEM_MIB * 1024 * 1024
        ),
        cost_estimate=pl.CostEstimate(
            flops=2 * n_dp * length * group * (HEAD * (d_q + length) + NOPE * D_KV),
            bytes_accessed=2 * rows * heads * HEAD, transcendentals=0,
        ),
        name="maxima",
    )(
        *[
            pltpu.with_memory_space_constraint(a, pltpu.HBM)
            for a in (
                q_latent[0], kv_latent[0].T, segment_ids.reshape(1, length), q_weight[0],
                k_weight[0], jnp.asarray(rope_tables(length)),
            )
        ],
    )
    ratio, scaled_q, scaled_k = pl.pallas_call(
        functools.partial(scale_kernel, n_sec),
        out_shape=(
            jax.ShapeDtypeStruct((n_sec, heads), jnp.float32),
            jax.ShapeDtypeStruct(q_weight.shape[1:], bf16),
            jax.ShapeDtypeStruct(k_weight.shape[1:], bf16),
        ),
        in_specs=[pl.BlockSpec(memory_space=pltpu.VMEM)] * 3,
        out_specs=[pl.BlockSpec(memory_space=pltpu.VMEM)]
        + [pl.BlockSpec(memory_space=pltpu.HBM)] * 2,
        scratch_shapes=[
            pltpu.VMEM(q_weight.shape[1:], bf16),
            pltpu.VMEM(k_weight.shape[1:], bf16),
            pltpu.VMEM((1, q_weight.shape[2]), jnp.float32),
            pltpu.VMEM((1, k_weight.shape[2]), jnp.float32),
            dma((8,)),
            dma((8,)),
        ],
        compiler_params=pltpu.CompilerParams(vmem_limit_bytes=24 * 1024 * 1024),
        cost_estimate=pl.CostEstimate(
            flops=rows * heads * HEAD, bytes_accessed=8 * rows * heads * HEAD, transcendentals=0
        ),
        name="scale",
    )(table, q_weight[0], k_weight[0])
    return ratio, scaled_q[None], scaled_k[None]


def per_device(sizes, q_latent, kv_latent, segment_ids, q_weight, k_weight):
    n_dp, n_sec, n_head = sizes
    heads = k_weight.shape[2] // NOPE
    length = q_latent.shape[1]
    exchange = (
        n_dp == 4 and n_sec % 2 == 0 and q_weight.shape[1] % 384 == 0 and n_head == 2 and heads == 8 * n_dp
        and length % 512 == 0 and q_latent.shape[0] == 1
    )
    args = (q_latent, kv_latent, segment_ids, q_weight, k_weight)
    if exchange:
        return exchanged((n_dp, n_sec), *args)
    own, max_table = gathered_maxima(*args)
    scaled_q, scaled_k = scale_weights(own, q_weight, k_weight)
    return max_table / clip_threshold, scaled_q, scaled_k


def solution(mesh):
    sizes = tuple(mesh.shape[axis] for axis in ("dp", "section", "head"))
    return jax.shard_map(
        functools.partial(per_device, sizes),
        mesh=mesh,
        in_specs=(
            P("section", "dp", None),
            P("section", "dp", None),
            P("dp"),
            P("section", "dp", "head"),
            P("section", None, "head"),
        ),
        out_specs=(P(None, "head"), P("section", "dp", "head"), P("section", None, "head")),
        check_vma=False,
    )
```

```python
import functools
import jax
import jax.numpy as jnp
import numpy as np
from jax import lax
from jax.experimental import pallas as pl
from jax.experimental.pallas import tpu as pltpu
from jax.sharding import PartitionSpec as P

D_KV = 512
NOPE = 128
ROPE = 64
HEAD = NOPE + ROPE
LANES = 128
NEG = -1e30
VMEM_MIB = 44
MESH = pl.DeviceIdType.MESH

clip_threshold = 100.0
rope_base = 50000.0


def rotate(values, positions):
    half_width = values.shape[-1] // 2
    frequency = rope_base ** (-jnp.arange(half_width, dtype=jnp.float32) / half_width)
    angles = positions[:, None].astype(jnp.float32) * frequency[None, :]
    cosine = jnp.cos(angles)[:, None, :]
    sine_part = jnp.sin(angles)[:, None, :]
    lower_half = values[..., :half_width]
    upper_half = values[..., half_width:]
    return jnp.concatenate(
        [
            lower_half * cosine - upper_half * sine_part,
            upper_half * cosine + lower_half * sine_part,
        ],
        -1,
    )


def sequence_maxima(q_full, kv_rows, segments, w_key):
    length = kv_rows.shape[0]
    heads_here = w_key.shape[1] // NOPE
    q_full = q_full.reshape(length, heads_here, HEAD)
    positions = jnp.arange(length, dtype=jnp.int32)
    queries = jnp.concatenate(
        [q_full[..., :NOPE], rotate(q_full[..., NOPE:], positions)], -1
    ).astype(jnp.bfloat16)
    key_nope = jnp.dot(kv_rows[:, :D_KV], w_key, preferred_element_type=jnp.float32).astype(
        jnp.bfloat16
    )
    key_nope = key_nope.reshape(length, heads_here, NOPE)
    key_rope = jnp.broadcast_to(kv_rows[:, None, D_KV:], (length, heads_here, ROPE))
    keys_all = jnp.concatenate([key_nope, key_rope], -1)
    logits = jnp.einsum("shd,thd->hst", queries, keys_all, preferred_element_type=jnp.float32)
    logits = logits * HEAD ** (-0.5)
    allowed = (segments[:, None] == segments[None, :]) & (positions[None, :] <= positions[:, None])
    return jnp.max(jnp.where(allowed[None], logits, NEG), axis=(1, 2))


def scale_weights(own_max, q_weight, k_weight):
    factor = clip_threshold / jnp.maximum(own_max, clip_threshold)
    square_root = jnp.sqrt(factor)
    layers, heads = own_max.shape
    q_columns = jnp.concatenate(
        [
            jnp.broadcast_to(square_root[..., None], (layers, heads, NOPE)),
            jnp.broadcast_to(factor[..., None], (layers, heads, ROPE)),
        ],
        -1,
    ).reshape(layers, 1, heads * HEAD)
    k_columns = jnp.broadcast_to(square_root[..., None], (layers, heads, NOPE)).reshape(
        layers, 1, heads * NOPE
    )
    scaled_q = (q_weight.astype(jnp.float32) * q_columns).astype(jnp.bfloat16)
    scaled_k = (k_weight.astype(jnp.float32) * k_columns).astype(jnp.bfloat16)
    return scaled_q, scaled_k


def gathered_maxima(q_latent, kv_latent, segment_ids, q_weight, k_weight):
    q_full = jnp.dot(
        q_latent[0],
        lax.all_gather(q_weight[0], "dp", axis=0, tiled=True),
        preferred_element_type=jnp.float32,
    )
    own_max = sequence_maxima(q_full, kv_latent[0], segment_ids, k_weight[0])[None]
    layer_max = lax.pmax(own_max, "dp")
    return layer_max, lax.all_gather(layer_max, "section", axis=0, tiled=True)


def rope_tables(length):
    half = ROPE // 2
    frequency = np.float32(rope_base) ** (-np.arange(half, dtype=np.float32) / np.float32(half))
    angles = np.arange(length, dtype=np.float32)[:, None] * frequency[None, :].astype(np.float32)
    cosine, sine = np.cos(angles), np.sin(angles)
    rest = np.zeros((length, ROPE), np.float32)
    low = [
        np.concatenate([cosine, cosine, rest + 1], 1),
        np.concatenate([-sine, sine, rest], 1),
    ]
    high = [np.roll(t, ROPE, 1) for t in low]
    return np.stack(low + high).astype(np.float32)


def maxima_kernel(
    n_sec, x_hbm, kv_hbm, seg_hbm, q_hbm, k_hbm, tab_hbm, out_ref,
    lat, kvt, seg, wq, wk, keys, bias, macc, tbuf, qacc, mid, mid2, tab_ref, outer_sem, line_sem, side_sem, all_sem, tab_sem,
    lat_recv, lat_send, seg_recv, seg_send, w_recv, w_send, k_recv, k_send, t_recv, t_send,
):
    n_seq, length, _ = lat.shape
    rows = q_hbm.shape[0]
    n_pair, d_q, pair = wq.shape
    group_q, group_k = n_pair * pair, wk.shape[1]
    part = length // 2
    last = n_pair - 1
    third = rows // 3
    pieces = [(p, 0, rows, 0, pair) for p in range(last)]
    pieces += [
        (last, 0, rows, 0, 2 * LANES),
        (last, 0, 2 * third, 2 * LANES, LANES),
        (last, 2 * third, third, 2 * LANES, LANES),
    ]

    z, sec, y = lax.axis_index("dp"), lax.axis_index("section"), lax.axis_index("head")
    c = lax.rem(sec, 2)
    half, z_low = z // 2, lax.rem(z, 2)
    base = sec - c
    primary = c == half
    core_peer = {"section": base + 1 - c}
    y_peer = {"head": 1 - y}
    z_peer = {"dp": 2 * half + 1 - z_low}
    entry = jnp.where(half == 0, 1, 2)
    me = z * n_sec + sec

    mid_z, outer_z = 3 - z, jnp.where(half == 0, 0, 3)
    inner = z == entry
    outer = jnp.logical_not(inner)
    both_cores = [base, base + 1]
    side_peers = [{"section": lax.rem(sec + 2 * i, n_sec)} for i in range(1, n_sec // 2)]
    side_peers.append(y_peer)

    def signal(sem, where):
        pl.semaphore_signal(sem, inc=1, device_id=where, device_id_type=MESH)

    barrier = pltpu.get_barrier_semaphore()

    @pl.when(inner)
    def _():
        for there in both_cores:
            signal(barrier, {"dp": mid_z, "section": there})
        for there in both_cores:
            signal(barrier, {"dp": outer_z, "section": there})

    @pl.when(outer)
    def _():
        for where in side_peers:
            signal(barrier, where)

    def local(src, dst, sem):
        return pltpu.make_async_copy(src, dst, sem)

    def ready(dst, sem):
        pltpu.make_async_copy(dst, dst, sem).wait()

    def remote(src, dst, send, recv, where):
        return pltpu.make_async_remote_copy(
            src_ref=src, dst_ref=dst, send_sem=send, recv_sem=recv,
            device_id=where, device_id_type=MESH,
        )

    def slots(seq, h):
        at = pl.ds(pl.multiple_of(h * part, part), part)
        return lat.at[seq, at, :], kvt.at[seq, :, at]

    def own(h):
        at = pl.ds(pl.multiple_of(h * part, part), part)
        return x_hbm.at[at, :], kv_hbm.at[:, at]

    def send(sources, seq, h, at, where, do):
        for i, (src, dst) in enumerate(zip(sources, slots(seq, h))):
            getattr(
                remote(src, dst, lat_send.at[at, i], lat_recv.at[seq, h, i], where), do
            )()

    def ready_half(seq, h):
        for i, dst in enumerate(slots(seq, h)):
            ready(dst, lat_recv.at[seq, h, i])

    own_group = 2 * z_low + c
    peer_group = 2 * z_low + 1 - c

    def group_columns(g):
        return k_hbm.at[:, pl.ds(pl.multiple_of(g * group_k, group_k), group_k)]

    def seg_copy(step):
        return remote(
            seg_hbm, seg.at[z], seg_send.at[step], seg_recv.at[z],
            {"dp": lax.rem(z + step, n_seq)},
        )

    def first_send(do):
        send(own(y), z, y, 0, {"dp": 3 - entry}, do)

    def own_sends(do):
        for step in range(1, n_seq):
            getattr(seg_copy(step), do)()

        @pl.when(jnp.logical_not(primary) & (outer if do == "start" else True))
        def _():
            first_send(do)

        @pl.when(primary)
        def _():
            send(own(y), z, y, 0, z_peer, do)
            for h in range(2):
                send(own(h), z, h, 1 + h, core_peer, do)
            k_peer = remote(group_columns(peer_group), wk, k_send, k_recv, core_peer)
            getattr(k_peer, do)()

    def rows_of(piece, source):
        p, first_row, count, first_column, width = pieces[piece]
        at = pl.ds(pl.multiple_of(source * rows + first_row, third), count)
        return wq.at[p, at, pl.ds(first_column, width)]

    def columns(piece, j, act):
        p, first_row, count, first_column, width = pieces[piece]
        if p < last:
            turn_to = lax.rem(j + 2 * z_low, 4)
        else:
            turn_to = 2 * (1 - c if j < 2 else c) + j % 2
        z_to, c_to = 2 * c + turn_to // 2, lax.rem(turn_to, 2)
        offset = pl.multiple_of(turn_to * group_q + p * pair + first_column, LANES)
        src = q_hbm.at[pl.ds(first_row, count), pl.ds(offset, width)]
        dst = rows_of(piece, z)
        mine = (z_to == z) & (c_to == c)
        there = {"dp": z_to, "section": base + c_to}
        if act == "start":
            @pl.when(mine)
            def _():
                local(src, dst, w_recv.at[piece, z]).start()

        @pl.when(jnp.logical_not(mine))
        def _():
            getattr(remote(src, dst, w_send.at[piece, j], w_recv.at[piece, z], there), act)()

    def send_columns(p):
        for j in range(4):
            columns(p, j, "start")

    def send_last_columns():
        for j in range(4):
            columns(last, j, "start")
        for first in (2, 0):
            for piece in range(last + 1, len(pieces)):
                for j in (first, first + 1):
                    columns(piece, j, "start")

    def wait_rows(piece, source):
        ready(rows_of(piece, source), w_recv.at[piece, source])

    pl.semaphore_wait(barrier, jnp.where(inner, 2, 2 + len(side_peers)))

    @pl.when(inner & jnp.logical_not(primary))
    def _():
        first_send("start")

    @pl.when(outer)
    def _():
        for there in both_cores:
            signal(outer_sem, {"dp": entry, "section": there})
        pl.semaphore_wait(line_sem, 1)

    @pl.when(inner)
    def _():
        pl.semaphore_wait(outer_sem, 2)
        signal(line_sem, {"dp": mid_z})
        pl.semaphore_wait(line_sem, 1)
        signal(line_sem, {"dp": outer_z})

    own_sends("start")
    local(seg_hbm, seg.at[z], seg_recv.at[z]).start()
    local(tab_hbm, tab_ref, tab_sem).start()

    @pl.when(primary)
    def _():
        for h in range(2):
            for i, (src, dst) in enumerate(zip(own(h), slots(z, h))):
                local(src, dst, lat_recv.at[z, h, i]).start()
        local(group_columns(own_group), wk, k_recv).start()

    send_columns(0)
    send_columns(1)

    @pl.when(outer)
    def _():
        for where in side_peers:
            signal(side_sem, where)
        pl.semaphore_wait(side_sem, len(side_peers))
        signal(all_sem, {"dp": entry})

    @pl.when(inner)
    def _():
        pl.semaphore_wait(all_sem, 1)

    others = [2 * half + 1 - z_low, jnp.where(half == 0, 2, 1), jnp.where(half == 0, 3, 0)]
    at_entry = z == entry

    def relay_first(i, seq, do):
        if i > 0:
            @pl.when(at_entry)
            def _():
                send(slots(seq, y), seq, y, 6 + 4 * i, z_peer, do)
        send(slots(seq, y), seq, y, 5 + 4 * i, y_peer, do)
        send(slots(seq, y), seq, y, 3 + 4 * i, core_peer, do)

    def relay_second(i, seq, do):
        send(slots(seq, 1 - y), seq, 1 - y, 4 + 4 * i, core_peer, do)

    @pl.when(primary)
    def _():
        for i, seq in enumerate(others):
            ready_half(seq, y)
            relay_first(i, seq, "start")
        for i, seq in enumerate(others):
            ready_half(seq, 1 - y)
            relay_second(i, seq, "start")
        for h in range(2):
            ready_half(z, h)

    for p in range(2, last):
        send_columns(p)
    send_last_columns()

    @pl.when(jnp.logical_not(primary))
    def _():
        for seq in range(n_seq):
            for h in range(2):
                ready_half(seq, h)

    ready(wk, k_recv)
    ready(tab_ref, tab_sem)
    for seq in range(n_seq):
        ready(seg.at[seq], seg_recv.at[seq])

    macc[...] = jnp.full(macc.shape, NEG, jnp.float32)

    def seq_keys(s, carry):
        seg_row = seg[s].astype(jnp.float32)
        seg_col = jnp.broadcast_to(seg_row, (LANES, length)).T[:, :1]
        row = lax.broadcasted_iota(jnp.int32, (length, length), 0)
        col = lax.broadcasted_iota(jnp.int32, (length, length), 1)
        bias[s] = jnp.where((seg_col == seg_row) & (col <= row), 0.0, NEG)
        rope = kvt[s, D_KV:, :]
        none = jnp.zeros((ROPE, length), jnp.bfloat16)
        for p in range(n_pair):
            k2 = lax.dot_general(
                wk[:, p * 2 * NOPE:(p + 1) * 2 * NOPE], kvt[s, :D_KV, :],
                (((0,), (0,)), ((), ())), preferred_element_type=jnp.float32,
            ).astype(jnp.bfloat16)
            keys[s, p, 0, :NOPE, :] = k2[:NOPE]
            keys[s, p, 0, NOPE:HEAD, :] = rope
            keys[s, p, 0, HEAD:, :] = none
            keys[s, p, 1, :ROPE, :] = none
            keys[s, p, 1, ROPE:HEAD, :] = k2[NOPE:]
            keys[s, p, 1, HEAD:, :] = rope
        return carry

    lax.fori_loop(0, n_seq, seq_keys, 0)

    lower = lax.rem(lax.broadcasted_iota(jnp.int32, (1, LANES), 1), ROPE) < ROPE // 2

    def turn(values, at):
        swapped = jnp.where(
            lower, pltpu.roll(values, LANES - ROPE // 2, 1), pltpu.roll(values, ROPE // 2, 1)
        )
        return (values * tab_ref[at] + swapped * tab_ref[at + 1]).astype(jnp.bfloat16)

    def tops(p, e, s, tiles):
        queries = jnp.concatenate(tiles, 1)
        found = []
        for block in range(2):
            lo, hi = block * part, (block + 1) * part
            logits = jnp.dot(
                queries[lo:, :], keys[s, p, e, :, lo:hi], preferred_element_type=jnp.float32
            ) + bias[s, lo:, lo:hi]
            found.append(jnp.max(logits.reshape((length - lo) // 8, 8, part), axis=0))
        return found

    def keep(p, e, found):
        for block, top in enumerate(found):
            at = slice(block * part, (block + 1) * part)
            macc[2 * p + e, :, at] = jnp.maximum(macc[2 * p + e, :, at], top)

    def head_maxima(p, e, s, tiles):
        keep(p, e, tops(p, e, s, tiles))

    def pair_maxima(p, s, q2):
        first = q2[:, :NOPE].astype(jnp.bfloat16)
        middle = turn(q2[:, NOPE:2 * NOPE], 0)
        head_maxima(p, 0, s, (first, middle))
        head_maxima(p, 1, s, (middle, turn(q2[:, 2 * NOPE:], 2)))

    def pair_logits(p, carry):
        for source in range(n_seq):
            at = pl.ds(source * rows, rows)
            ready(wq.at[p, at, :], w_recv.at[p, source])

        def one(s, inner):
            pair_maxima(p, s, jnp.dot(lat[s], wq[p], preferred_element_type=jnp.float32))
            return inner

        return lax.fori_loop(0, n_seq, one, carry)

    lax.fori_loop(0, last, pair_logits, 0)

    def partial(s, starts, count, first_column, width):
        spans = [pl.ds(pl.multiple_of(start, third), count) for start in starts]
        tokens = [lat[s, :, at] for at in spans]
        weights = [wq[last, at, pl.ds(first_column, width)] for at in spans]
        if len(spans) > 1:
            tokens, weights = [jnp.concatenate(tokens, 1)], [jnp.concatenate(weights, 0)]
        return jnp.dot(tokens[0], weights[0], preferred_element_type=jnp.float32)

    near_sources = [2 * half, 2 * half + 1]
    far_sources = [2 * (1 - half), 2 * (1 - half) + 1]
    far_rows = [source * rows for source in far_sources]
    whole, narrow = last, slice(2 * LANES, 3 * LANES)

    def from_near(s, carry):
        qacc[s] = partial(s, [near_sources[0] * rows], 2 * rows, 0, pair)
        return carry

    def from_far(s, carry):
        q2 = qacc[s, :, :2 * LANES] + partial(s, far_rows[:1], 2 * rows, 0, 2 * LANES)
        middle = turn(q2[:, LANES:], 0)
        mid[s] = middle
        head_maxima(last, 0, s, (q2[:, :LANES].astype(jnp.bfloat16), middle))
        return carry

    def from_far_tile(s, carry):
        qacc[s, :, narrow] = qacc[s, :, narrow] + partial(
            s, far_rows, 2 * third, 2 * LANES, LANES
        )
        return carry

    def finish(s):
        starts = [start + 2 * third for start in far_rows]
        q1 = qacc[s, :, narrow] + partial(s, starts, third, 2 * LANES, LANES)
        mid2[s] = turn(q1, 2)

    for source in near_sources:
        for piece in range(last, len(pieces)):
            wait_rows(piece, source)
    lax.fori_loop(0, n_seq, from_near, 0)
    for source in far_sources:
        wait_rows(whole, source)
    lax.fori_loop(0, n_seq, from_far, 0)
    for source in far_sources:
        wait_rows(last + 1, source)
    for s in range(n_seq):
        from_far_tile(s, 0)
    for source in far_sources:
        wait_rows(last + 2, source)
    for s in range(n_seq):
        finish(s)
    found = [tops(last, 1, s, (mid[s], mid2[s])) for s in range(n_seq)]
    keep(last, 1, [functools.reduce(jnp.maximum, tops_of) for tops_of in zip(*found)])

    top = jnp.max(jnp.max(macc[...], axis=1), axis=1, keepdims=True) * HEAD ** (-0.5)
    tile = jnp.broadcast_to(top, tbuf.shape)
    tbuf[...] = tile
    out_ref[me] = tile

    def table_copy(step):
        other = lax.rem(me + step, n_seq * n_sec)
        return remote(
            tbuf, out_ref.at[me], t_send.at[step], t_recv.at[me],
            {"dp": other // n_sec, "section": lax.rem(other, n_sec)},
        )

    for step in range(1, n_seq * n_sec):
        table_copy(step).start()
    for piece in range(len(pieces)):
        for j in range(4):
            columns(piece, j, "wait_send")
    own_sends("wait_send")

    @pl.when(primary)
    def _():
        for i, seq in enumerate(others):
            relay_first(i, seq, "wait_send")
            relay_second(i, seq, "wait_send")

    for step in range(1, n_seq * n_sec):
        source = lax.rem(me + step, n_seq * n_sec)
        ready(out_ref.at[source], t_recv.at[source])
    for step in range(1, n_seq * n_sec):
        table_copy(step).wait_send()


def scale_kernel(
    n_sec, table, q_ref, k_ref, ratio_out, q_out, k_out, q_buf, k_buf, q_row, k_row, ratio_ref,
    q_sem, k_sem, ratio_sem,
):
    group = table.shape[1]
    n_group, n_pair = q_ref.shape[1] // (group * HEAD), group // 2
    n_chunk = q_sem.shape[0]
    sec = lax.axis_index("section")
    low = lax.broadcasted_iota(jnp.int32, (1, LANES), 1) < ROPE

    def slot(layer, number):
        z_of = 2 * (layer % 2) + number // 2
        return z_of * n_sec + 2 * (layer // 2) + number % 2

    for g in range(n_group):
        factor = clip_threshold / jnp.maximum(table[slot(sec, g)], clip_threshold)
        root = jnp.sqrt(factor)
        for p in range(n_pair):
            f_a, f_b = factor[2 * p:2 * p + 1], factor[2 * p + 1:2 * p + 2]
            r_a, r_b = root[2 * p:2 * p + 1], root[2 * p + 1:2 * p + 2]
            number = g * n_pair + p
            scales = (r_a, jnp.where(low, f_a, r_b), jnp.where(low, r_b, f_b))
            for i, scale in enumerate(scales):
                q_row[:, pl.ds((3 * number + i) * LANES, LANES)] = scale
            for i, scale in enumerate((r_a, r_b)):
                k_row[:, pl.ds((2 * number + i) * LANES, LANES)] = scale

    def block(source, target, sem, i):
        count = source.shape[0] // n_chunk
        at = pl.ds(pl.multiple_of(i * count, count), count)
        return at, pltpu.make_async_copy(source.at[at, :], target.at[at, :], sem.at[i])

    def one_chunk(i, carry):
        for source, row, buf, target, sem in (
            (q_ref, q_row, q_buf, q_out, q_sem), (k_ref, k_row, k_buf, k_out, k_sem),
        ):
            at, copy = block(buf, target, sem, i)
            for tile in range(source.shape[1] // LANES):
                lanes = pl.ds(tile * LANES, LANES)
                values = source[at, lanes].astype(jnp.float32) * row[:, lanes]
                buf[at, lanes] = values.astype(jnp.bfloat16)
            copy.start()
        return carry

    lax.fori_loop(0, n_chunk, one_chunk, 0)

    lane = lax.broadcasted_iota(jnp.int32, (group, LANES), 1)
    place = lax.broadcasted_iota(jnp.int32, (group, LANES), 0)
    for layer in range(ratio_ref.shape[0]):
        line = jnp.zeros((1, LANES), jnp.float32)
        for number in range(n_group):
            values = table[slot(layer, number)]
            here = lane == number * group + place
            line = line + jnp.sum(jnp.where(here, values, 0.0), axis=0, keepdims=True)
        ratio_ref[layer:layer + 1, :] = line[:, :ratio_ref.shape[1]] / clip_threshold

    ratio_copy = pltpu.make_async_copy(ratio_ref, ratio_out, ratio_sem)
    ratio_copy.start()
    for i in range(n_chunk):
        block(q_buf, q_out, q_sem, i)[1].wait()
        block(k_buf, k_out, k_sem, i)[1].wait()
    ratio_copy.wait()


def exchanged(sizes, q_latent, kv_latent, segment_ids, q_weight, k_weight):
    n_dp, n_sec = sizes
    _, length, d_q = q_latent.shape
    rows = q_weight.shape[1]
    heads = k_weight.shape[2] // NOPE
    group = heads // n_dp
    n_pair = group // 2
    bf16, dma = jnp.bfloat16, pltpu.SemaphoreType.DMA
    n_all = n_dp * n_sec
    table = pl.pallas_call(
        functools.partial(maxima_kernel, n_sec),
        out_shape=jax.ShapeDtypeStruct((n_all, group, LANES), jnp.float32),
        in_specs=[pl.BlockSpec(memory_space=pltpu.HBM)] * 6,
        out_specs=pl.BlockSpec(memory_space=pltpu.VMEM),
        scratch_shapes=[
            pltpu.VMEM((n_dp, length, d_q), bf16),
            pltpu.VMEM((n_dp, D_KV + ROPE, length), bf16),
            pltpu.VMEM((n_dp, 1, length), jnp.int32),
            pltpu.VMEM((n_pair, d_q, 2 * HEAD), bf16),
            pltpu.VMEM((D_KV, group * NOPE), bf16),
            pltpu.VMEM((n_dp, n_pair, 2, 2 * NOPE, length), bf16),
            pltpu.VMEM((n_dp, length, length), jnp.float32),
            pltpu.VMEM((group, 8, length), jnp.float32),
            pltpu.VMEM((group, LANES), jnp.float32),
            pltpu.VMEM((n_dp, length, 2 * HEAD), jnp.float32),
            pltpu.VMEM((n_dp, length, LANES), bf16),
            pltpu.VMEM((n_dp, length, LANES), bf16),
            pltpu.VMEM((4, length, LANES), jnp.float32),
            *[pltpu.SemaphoreType.REGULAR] * 4,
            dma,
            dma((n_dp, 2, 2)),
            dma((15, 2)),
            dma((n_dp,)),
            dma((n_dp,)),
            dma((n_pair + 2, n_dp)),
            dma((n_pair + 2, 4)),
            dma,
            dma,
            dma((n_all,)),
            dma((n_all,)),
        ],
        compiler_params=pltpu.CompilerParams(
            collective_id=0, has_side_effects=True, vmem_limit_bytes=VMEM_MIB * 1024 * 1024
        ),
        cost_estimate=pl.CostEstimate(
            flops=2 * n_dp * length * group * (HEAD * (d_q + length) + NOPE * D_KV),
            bytes_accessed=2 * rows * heads * HEAD, transcendentals=0,
        ),
        name="maxima",
    )(
        *[
            pltpu.with_memory_space_constraint(a, pltpu.HBM)
            for a in (
                q_latent[0], kv_latent[0].T, segment_ids.reshape(1, length), q_weight[0],
                k_weight[0], jnp.asarray(rope_tables(length)),
            )
        ],
    )
    ratio, scaled_q, scaled_k = pl.pallas_call(
        functools.partial(scale_kernel, n_sec),
        out_shape=(
            jax.ShapeDtypeStruct((n_sec, heads), jnp.float32),
            jax.ShapeDtypeStruct(q_weight.shape[1:], bf16),
            jax.ShapeDtypeStruct(k_weight.shape[1:], bf16),
        ),
        in_specs=[pl.BlockSpec(memory_space=pltpu.VMEM)] * 3,
        out_specs=[pl.BlockSpec(memory_space=pltpu.HBM)] * 3,
        scratch_shapes=[
            pltpu.VMEM(q_weight.shape[1:], bf16),
            pltpu.VMEM(k_weight.shape[1:], bf16),
            pltpu.VMEM((1, q_weight.shape[2]), jnp.float32),
            pltpu.VMEM((1, k_weight.shape[2]), jnp.float32),
            pltpu.VMEM((n_sec, heads), jnp.float32),
            dma((8,)),
            dma((8,)),
            dma,
        ],
        compiler_params=pltpu.CompilerParams(vmem_limit_bytes=24 * 1024 * 1024),
        cost_estimate=pl.CostEstimate(
            flops=rows * heads * HEAD, bytes_accessed=8 * rows * heads * HEAD, transcendentals=0
        ),
        name="scale",
    )(table, q_weight[0], k_weight[0])
    return ratio, scaled_q[None], scaled_k[None]


def per_device(sizes, q_latent, kv_latent, segment_ids, q_weight, k_weight):
    n_dp, n_sec, n_head = sizes
    heads = k_weight.shape[2] // NOPE
    length = q_latent.shape[1]
    exchange = (
        n_dp == 4 and n_sec % 2 == 0 and q_weight.shape[1] % 384 == 0 and n_head == 2 and heads == 8 * n_dp
        and length % 512 == 0 and q_latent.shape[0] == 1
    )
    args = (q_latent, kv_latent, segment_ids, q_weight, k_weight)
    if exchange:
        return exchanged((n_dp, n_sec), *args)
    own, max_table = gathered_maxima(*args)
    scaled_q, scaled_k = scale_weights(own, q_weight, k_weight)
    return max_table / clip_threshold, scaled_q, scaled_k


def solution(mesh):
    sizes = tuple(mesh.shape[axis] for axis in ("dp", "section", "head"))
    return jax.shard_map(
        functools.partial(per_device, sizes),
        mesh=mesh,
        in_specs=(
            P("section", "dp", None),
            P("section", "dp", None),
            P("dp"),
            P("section", "dp", "head"),
            P("section", None, "head"),
        ),
        out_specs=(P(None, "head"), P("section", "dp", "head"), P("section", None, "head")),
        check_vma=False,
    )
```

```python
import functools
import jax
import jax.numpy as jnp
import numpy as np
from jax import lax
from jax.experimental import pallas as pl
from jax.experimental.pallas import tpu as pltpu
from jax.sharding import PartitionSpec as P

D_KV = 512
NOPE = 128
ROPE = 64
HEAD = NOPE + ROPE
LANES = 128
NEG = -1e30
VMEM_MIB = 44
MESH = pl.DeviceIdType.MESH

clip_threshold = 100.0
rope_base = 50000.0


def rotate(values, positions):
    half_width = values.shape[-1] // 2
    frequency = rope_base ** (-jnp.arange(half_width, dtype=jnp.float32) / half_width)
    angles = positions[:, None].astype(jnp.float32) * frequency[None, :]
    cosine = jnp.cos(angles)[:, None, :]
    sine_part = jnp.sin(angles)[:, None, :]
    lower_half = values[..., :half_width]
    upper_half = values[..., half_width:]
    return jnp.concatenate(
        [
            lower_half * cosine - upper_half * sine_part,
            upper_half * cosine + lower_half * sine_part,
        ],
        -1,
    )


def sequence_maxima(q_full, kv_rows, segments, w_key):
    length = kv_rows.shape[0]
    heads_here = w_key.shape[1] // NOPE
    q_full = q_full.reshape(length, heads_here, HEAD)
    positions = jnp.arange(length, dtype=jnp.int32)
    queries = jnp.concatenate(
        [q_full[..., :NOPE], rotate(q_full[..., NOPE:], positions)], -1
    ).astype(jnp.bfloat16)
    key_nope = jnp.dot(kv_rows[:, :D_KV], w_key, preferred_element_type=jnp.float32).astype(
        jnp.bfloat16
    )
    key_nope = key_nope.reshape(length, heads_here, NOPE)
    key_rope = jnp.broadcast_to(kv_rows[:, None, D_KV:], (length, heads_here, ROPE))
    keys_all = jnp.concatenate([key_nope, key_rope], -1)
    logits = jnp.einsum("shd,thd->hst", queries, keys_all, preferred_element_type=jnp.float32)
    logits = logits * HEAD ** (-0.5)
    allowed = (segments[:, None] == segments[None, :]) & (positions[None, :] <= positions[:, None])
    return jnp.max(jnp.where(allowed[None], logits, NEG), axis=(1, 2))


def scale_weights(own_max, q_weight, k_weight):
    factor = clip_threshold / jnp.maximum(own_max, clip_threshold)
    square_root = jnp.sqrt(factor)
    layers, heads = own_max.shape
    q_columns = jnp.concatenate(
        [
            jnp.broadcast_to(square_root[..., None], (layers, heads, NOPE)),
            jnp.broadcast_to(factor[..., None], (layers, heads, ROPE)),
        ],
        -1,
    ).reshape(layers, 1, heads * HEAD)
    k_columns = jnp.broadcast_to(square_root[..., None], (layers, heads, NOPE)).reshape(
        layers, 1, heads * NOPE
    )
    scaled_q = (q_weight.astype(jnp.float32) * q_columns).astype(jnp.bfloat16)
    scaled_k = (k_weight.astype(jnp.float32) * k_columns).astype(jnp.bfloat16)
    return scaled_q, scaled_k


def gathered_maxima(q_latent, kv_latent, segment_ids, q_weight, k_weight):
    q_full = jnp.dot(
        q_latent[0],
        lax.all_gather(q_weight[0], "dp", axis=0, tiled=True),
        preferred_element_type=jnp.float32,
    )
    own_max = sequence_maxima(q_full, kv_latent[0], segment_ids, k_weight[0])[None]
    layer_max = lax.pmax(own_max, "dp")
    return layer_max, lax.all_gather(layer_max, "section", axis=0, tiled=True)


def rope_tables(length):
    half = ROPE // 2
    frequency = np.float32(rope_base) ** (-np.arange(half, dtype=np.float32) / np.float32(half))
    angles = np.arange(length, dtype=np.float32)[:, None] * frequency[None, :].astype(np.float32)
    cosine, sine = np.cos(angles), np.sin(angles)
    rest = np.zeros((length, ROPE), np.float32)
    low = [
        np.concatenate([cosine, cosine, rest + 1], 1),
        np.concatenate([-sine, sine, rest], 1),
    ]
    high = [np.roll(t, ROPE, 1) for t in low]
    return np.stack(low + high).astype(np.float32)


def maxima_kernel(
    n_sec, x_hbm, kv_hbm, seg_hbm, q_hbm, k_hbm, tab_hbm, out_ref,
    lat, kvt, seg, wq, wk, keys, bias, macc, tbuf, qacc, mid, mid2, tab_ref, outer_sem, line_sem, side_sem, all_sem, tab_sem,
    lat_recv, lat_send, seg_recv, seg_send, w_recv, w_send, k_recv, k_send, t_recv, t_send,
):
    n_seq, length, _ = lat.shape
    rows = q_hbm.shape[0]
    n_pair, d_q, pair = wq.shape
    group_q, group_k = n_pair * pair, wk.shape[1]
    part = length // 2
    last = n_pair - 1
    third = rows // 3
    pieces = [(p, 0, rows, 0, pair) for p in range(last)]
    pieces += [
        (last, 0, rows, 0, 2 * LANES),
        (last, 0, 2 * third, 2 * LANES, LANES),
        (last, 2 * third, third, 2 * LANES, LANES),
    ]

    z, sec, y = lax.axis_index("dp"), lax.axis_index("section"), lax.axis_index("head")
    c = lax.rem(sec, 2)
    half, z_low = z // 2, lax.rem(z, 2)
    base = sec - c
    primary = c == half
    core_peer = {"section": base + 1 - c}
    y_peer = {"head": 1 - y}
    z_peer = {"dp": 2 * half + 1 - z_low}
    entry = jnp.where(half == 0, 1, 2)
    me = z * n_sec + sec

    mid_z, outer_z = 3 - z, jnp.where(half == 0, 0, 3)
    inner = z == entry
    outer = jnp.logical_not(inner)
    both_cores = [base, base + 1]
    side_peers = [{"section": lax.rem(sec + 2 * i, n_sec)} for i in range(1, n_sec // 2)]
    side_peers.append(y_peer)

    def signal(sem, where):
        pl.semaphore_signal(sem, inc=1, device_id=where, device_id_type=MESH)

    barrier = pltpu.get_barrier_semaphore()

    @pl.when(inner)
    def _():
        signal(barrier, {"dp": mid_z})
        for there in both_cores:
            signal(barrier, {"dp": outer_z, "section": there})

    @pl.when(outer)
    def _():
        for where in side_peers:
            signal(barrier, where)

    def local(src, dst, sem):
        return pltpu.make_async_copy(src, dst, sem)

    def ready(dst, sem):
        pltpu.make_async_copy(dst, dst, sem).wait()

    def remote(src, dst, send, recv, where):
        return pltpu.make_async_remote_copy(
            src_ref=src, dst_ref=dst, send_sem=send, recv_sem=recv,
            device_id=where, device_id_type=MESH,
        )

    def slots(seq, h):
        at = pl.ds(pl.multiple_of(h * part, part), part)
        return lat.at[seq, at, :], kvt.at[seq, :, at]

    def own(h):
        at = pl.ds(pl.multiple_of(h * part, part), part)
        return x_hbm.at[at, :], kv_hbm.at[:, at]

    def send(sources, seq, h, at, where, do):
        for i, (src, dst) in enumerate(zip(sources, slots(seq, h))):
            getattr(
                remote(src, dst, lat_send.at[at, i], lat_recv.at[seq, h, i], where), do
            )()

    def ready_half(seq, h):
        for i, dst in enumerate(slots(seq, h)):
            ready(dst, lat_recv.at[seq, h, i])

    own_group = 2 * z_low + c
    peer_group = 2 * z_low + 1 - c

    def group_columns(g):
        return k_hbm.at[:, pl.ds(pl.multiple_of(g * group_k, group_k), group_k)]

    def seg_copy(step):
        return remote(
            seg_hbm, seg.at[z], seg_send.at[step], seg_recv.at[z],
            {"dp": lax.rem(z + step, n_seq)},
        )

    def first_send(do):
        send(own(y), z, y, 0, {"dp": 3 - entry}, do)

    def own_sends(do):
        for step in range(1, n_seq):
            getattr(seg_copy(step), do)()

        @pl.when(jnp.logical_not(primary) & (outer if do == "start" else True))
        def _():
            first_send(do)

        @pl.when(primary)
        def _():
            send(own(y), z, y, 0, z_peer, do)
            for h in range(2):
                send(own(h), z, h, 1 + h, core_peer, do)
            k_peer = remote(group_columns(peer_group), wk, k_send, k_recv, core_peer)
            getattr(k_peer, do)()

    def rows_of(piece, source):
        p, first_row, count, first_column, width = pieces[piece]
        at = pl.ds(pl.multiple_of(source * rows + first_row, third), count)
        return wq.at[p, at, pl.ds(first_column, width)]

    def columns(piece, j, act):
        p, first_row, count, first_column, width = pieces[piece]
        if p < last:
            turn_to = lax.rem(j + 2 * z_low, 4)
        else:
            turn_to = 2 * (1 - c if j < 2 else c) + j % 2
        z_to, c_to = 2 * c + turn_to // 2, lax.rem(turn_to, 2)
        offset = pl.multiple_of(turn_to * group_q + p * pair + first_column, LANES)
        src = q_hbm.at[pl.ds(first_row, count), pl.ds(offset, width)]
        dst = rows_of(piece, z)
        mine = (z_to == z) & (c_to == c)
        there = {"dp": z_to, "section": base + c_to}
        if act == "start":
            @pl.when(mine)
            def _():
                local(src, dst, w_recv.at[piece, z]).start()

        @pl.when(jnp.logical_not(mine))
        def _():
            getattr(remote(src, dst, w_send.at[piece, j], w_recv.at[piece, z], there), act)()

    def send_columns(p):
        for j in range(4):
            columns(p, j, "start")

    def send_last_columns():
        for j in range(4):
            columns(last, j, "start")
        for first in (2, 0):
            for piece in range(last + 1, len(pieces)):
                for j in (first, first + 1):
                    columns(piece, j, "start")

    def wait_rows(piece, source):
        ready(rows_of(piece, source), w_recv.at[piece, source])

    pl.semaphore_wait(barrier, jnp.where(inner, 1, 2 + len(side_peers)))

    @pl.when(inner & jnp.logical_not(primary))
    def _():
        first_send("start")

    @pl.when(outer)
    def _():
        for there in both_cores:
            signal(outer_sem, {"dp": entry, "section": there})
        pl.semaphore_wait(line_sem, 1)

    @pl.when(inner)
    def _():
        pl.semaphore_wait(outer_sem, 2)
        signal(line_sem, {"dp": mid_z})
        pl.semaphore_wait(line_sem, 1)
        signal(line_sem, {"dp": outer_z})

    own_sends("start")
    local(seg_hbm, seg.at[z], seg_recv.at[z]).start()
    local(tab_hbm, tab_ref, tab_sem).start()

    @pl.when(primary)
    def _():
        for h in range(2):
            for i, (src, dst) in enumerate(zip(own(h), slots(z, h))):
                local(src, dst, lat_recv.at[z, h, i]).start()
        local(group_columns(own_group), wk, k_recv).start()

    send_columns(0)
    send_columns(1)

    @pl.when(outer)
    def _():
        for where in side_peers:
            signal(side_sem, where)
        pl.semaphore_wait(side_sem, len(side_peers))
        signal(all_sem, {"dp": entry})

    @pl.when(inner)
    def _():
        pl.semaphore_wait(all_sem, 1)

    others = [2 * half + 1 - z_low, jnp.where(half == 0, 2, 1), jnp.where(half == 0, 3, 0)]
    at_entry = z == entry

    def relay_first(i, seq, do):
        if i > 0:
            @pl.when(at_entry)
            def _():
                send(slots(seq, y), seq, y, 6 + 4 * i, z_peer, do)
        send(slots(seq, y), seq, y, 5 + 4 * i, y_peer, do)
        send(slots(seq, y), seq, y, 3 + 4 * i, core_peer, do)

    def relay_second(i, seq, do):
        send(slots(seq, 1 - y), seq, 1 - y, 4 + 4 * i, core_peer, do)

    @pl.when(primary)
    def _():
        for i, seq in enumerate(others):
            ready_half(seq, y)
            relay_first(i, seq, "start")
        for i, seq in enumerate(others):
            ready_half(seq, 1 - y)
            relay_second(i, seq, "start")
        for h in range(2):
            ready_half(z, h)

    for p in range(2, last):
        send_columns(p)
    send_last_columns()

    @pl.when(jnp.logical_not(primary))
    def _():
        for seq in range(n_seq):
            for h in range(2):
                ready_half(seq, h)

    ready(wk, k_recv)
    ready(tab_ref, tab_sem)
    for seq in range(n_seq):
        ready(seg.at[seq], seg_recv.at[seq])

    macc[...] = jnp.full(macc.shape, NEG, jnp.float32)

    def seq_keys(s, carry):
        seg_row = seg[s].astype(jnp.float32)
        seg_col = jnp.broadcast_to(seg_row, (LANES, length)).T[:, :1]
        row = lax.broadcasted_iota(jnp.int32, (length, length), 0)
        col = lax.broadcasted_iota(jnp.int32, (length, length), 1)
        bias[s] = jnp.where((seg_col == seg_row) & (col <= row), 0.0, NEG)
        rope = kvt[s, D_KV:, :]
        none = jnp.zeros((ROPE, length), jnp.bfloat16)
        for p in range(n_pair):
            k2 = lax.dot_general(
                wk[:, p * 2 * NOPE:(p + 1) * 2 * NOPE], kvt[s, :D_KV, :],
                (((0,), (0,)), ((), ())), preferred_element_type=jnp.float32,
            ).astype(jnp.bfloat16)
            keys[s, p, 0, :NOPE, :] = k2[:NOPE]
            keys[s, p, 0, NOPE:HEAD, :] = rope
            keys[s, p, 0, HEAD:, :] = none
            keys[s, p, 1, :ROPE, :] = none
            keys[s, p, 1, ROPE:HEAD, :] = k2[NOPE:]
            keys[s, p, 1, HEAD:, :] = rope
        return carry

    lax.fori_loop(0, n_seq, seq_keys, 0)

    lower = lax.rem(lax.broadcasted_iota(jnp.int32, (1, LANES), 1), ROPE) < ROPE // 2

    def turn(values, at):
        swapped = jnp.where(
            lower, pltpu.roll(values, LANES - ROPE // 2, 1), pltpu.roll(values, ROPE // 2, 1)
        )
        return (values * tab_ref[at] + swapped * tab_ref[at + 1]).astype(jnp.bfloat16)

    def tops(p, e, s, tiles):
        queries = jnp.concatenate(tiles, 1)
        found = []
        for block in range(2):
            lo, hi = block * part, (block + 1) * part
            logits = jnp.dot(
                queries[lo:, :], keys[s, p, e, :, lo:hi], preferred_element_type=jnp.float32
            ) + bias[s, lo:, lo:hi]
            found.append(jnp.max(logits.reshape((length - lo) // 8, 8, part), axis=0))
        return found

    def keep(p, e, found):
        for block, top in enumerate(found):
            at = slice(block * part, (block + 1) * part)
            macc[2 * p + e, :, at] = jnp.maximum(macc[2 * p + e, :, at], top)

    def head_maxima(p, e, s, tiles):
        keep(p, e, tops(p, e, s, tiles))

    def pair_maxima(p, s, q2):
        first = q2[:, :NOPE].astype(jnp.bfloat16)
        middle = turn(q2[:, NOPE:2 * NOPE], 0)
        head_maxima(p, 0, s, (first, middle))
        head_maxima(p, 1, s, (middle, turn(q2[:, 2 * NOPE:], 2)))

    def pair_logits(p, carry):
        for source in range(n_seq):
            at = pl.ds(source * rows, rows)
            ready(wq.at[p, at, :], w_recv.at[p, source])

        def one(s, inner):
            pair_maxima(p, s, jnp.dot(lat[s], wq[p], preferred_element_type=jnp.float32))
            return inner

        return lax.fori_loop(0, n_seq, one, carry)

    lax.fori_loop(0, last, pair_logits, 0)

    def partial(s, starts, count, first_column, width):
        spans = [pl.ds(pl.multiple_of(start, third), count) for start in starts]
        tokens = [lat[s, :, at] for at in spans]
        weights = [wq[last, at, pl.ds(first_column, width)] for at in spans]
        if len(spans) > 1:
            tokens, weights = [jnp.concatenate(tokens, 1)], [jnp.concatenate(weights, 0)]
        return jnp.dot(tokens[0], weights[0], preferred_element_type=jnp.float32)

    near_sources = [2 * half, 2 * half + 1]
    far_sources = [2 * (1 - half), 2 * (1 - half) + 1]
    far_rows = [source * rows for source in far_sources]
    whole, narrow = last, slice(2 * LANES, 3 * LANES)

    def from_near(s, carry):
        qacc[s] = partial(s, [near_sources[0] * rows], 2 * rows, 0, pair)
        return carry

    def from_far(s, carry):
        q2 = qacc[s, :, :2 * LANES] + partial(s, far_rows[:1], 2 * rows, 0, 2 * LANES)
        middle = turn(q2[:, LANES:], 0)
        mid[s] = middle
        head_maxima(last, 0, s, (q2[:, :LANES].astype(jnp.bfloat16), middle))
        return carry

    def from_far_tile(s, carry):
        qacc[s, :, narrow] = qacc[s, :, narrow] + partial(
            s, far_rows, 2 * third, 2 * LANES, LANES
        )
        return carry

    def finish(s):
        starts = [start + 2 * third for start in far_rows]
        q1 = qacc[s, :, narrow] + partial(s, starts, third, 2 * LANES, LANES)
        mid2[s] = turn(q1, 2)

    for source in near_sources:
        for piece in range(last, len(pieces)):
            wait_rows(piece, source)
    lax.fori_loop(0, n_seq, from_near, 0)
    for source in far_sources:
        wait_rows(whole, source)
    lax.fori_loop(0, n_seq, from_far, 0)
    for source in far_sources:
        wait_rows(last + 1, source)
    for s in range(n_seq):
        from_far_tile(s, 0)
    for source in far_sources:
        wait_rows(last + 2, source)
    for s in range(n_seq):
        finish(s)
    found = [tops(last, 1, s, (mid[s], mid2[s])) for s in range(n_seq)]
    keep(last, 1, [functools.reduce(jnp.maximum, tops_of) for tops_of in zip(*found)])

    top = jnp.max(jnp.max(macc[...], axis=1), axis=1, keepdims=True) * HEAD ** (-0.5)
    tile = jnp.broadcast_to(top, tbuf.shape)
    tbuf[...] = tile
    out_ref[me] = tile

    def table_copy(step):
        other = lax.rem(me + step, n_seq * n_sec)
        return remote(
            tbuf, out_ref.at[me], t_send.at[step], t_recv.at[me],
            {"dp": other // n_sec, "section": lax.rem(other, n_sec)},
        )

    for step in range(1, n_seq * n_sec):
        table_copy(step).start()
    for piece in range(len(pieces)):
        for j in range(4):
            columns(piece, j, "wait_send")
    own_sends("wait_send")

    @pl.when(primary)
    def _():
        for i, seq in enumerate(others):
            relay_first(i, seq, "wait_send")
            relay_second(i, seq, "wait_send")

    for step in range(1, n_seq * n_sec):
        source = lax.rem(me + step, n_seq * n_sec)
        ready(out_ref.at[source], t_recv.at[source])
    for step in range(1, n_seq * n_sec):
        table_copy(step).wait_send()


def scale_kernel(
    n_sec, table, q_ref, k_ref, ratio_out, q_out, k_out, q_buf, k_buf, q_row, k_row, ratio_ref,
    q_sem, k_sem, ratio_sem,
):
    group = table.shape[1]
    n_group, n_pair = q_ref.shape[1] // (group * HEAD), group // 2
    n_chunk = q_sem.shape[0]
    sec = lax.axis_index("section")
    low = lax.broadcasted_iota(jnp.int32, (1, LANES), 1) < ROPE

    def slot(layer, number):
        z_of = 2 * (layer % 2) + number // 2
        return z_of * n_sec + 2 * (layer // 2) + number % 2

    for g in range(n_group):
        factor = clip_threshold / jnp.maximum(table[slot(sec, g)], clip_threshold)
        root = jnp.sqrt(factor)
        for p in range(n_pair):
            f_a, f_b = factor[2 * p:2 * p + 1], factor[2 * p + 1:2 * p + 2]
            r_a, r_b = root[2 * p:2 * p + 1], root[2 * p + 1:2 * p + 2]
            number = g * n_pair + p
            scales = (r_a, jnp.where(low, f_a, r_b), jnp.where(low, r_b, f_b))
            for i, scale in enumerate(scales):
                q_row[:, pl.ds((3 * number + i) * LANES, LANES)] = scale
            for i, scale in enumerate((r_a, r_b)):
                k_row[:, pl.ds((2 * number + i) * LANES, LANES)] = scale

    def block(source, target, sem, i):
        count = source.shape[0] // n_chunk
        at = pl.ds(pl.multiple_of(i * count, count), count)
        return at, pltpu.make_async_copy(source.at[at, :], target.at[at, :], sem.at[i])

    def one_chunk(i, carry):
        for source, row, buf, target, sem in (
            (q_ref, q_row, q_buf, q_out, q_sem), (k_ref, k_row, k_buf, k_out, k_sem),
        ):
            at, copy = block(buf, target, sem, i)
            for tile in range(source.shape[1] // LANES):
                lanes = pl.ds(tile * LANES, LANES)
                values = source[at, lanes].astype(jnp.float32) * row[:, lanes]
                buf[at, lanes] = values.astype(jnp.bfloat16)
            copy.start()
        return carry

    lax.fori_loop(0, n_chunk, one_chunk, 0)

    lane = lax.broadcasted_iota(jnp.int32, (group, LANES), 1)
    place = lax.broadcasted_iota(jnp.int32, (group, LANES), 0)
    for layer in range(ratio_ref.shape[0]):
        line = jnp.zeros((1, LANES), jnp.float32)
        for number in range(n_group):
            values = table[slot(layer, number)]
            here = lane == number * group + place
            line = line + jnp.sum(jnp.where(here, values, 0.0), axis=0, keepdims=True)
        ratio_ref[layer:layer + 1, :] = line[:, :ratio_ref.shape[1]] / clip_threshold

    ratio_copy = pltpu.make_async_copy(ratio_ref, ratio_out, ratio_sem)
    ratio_copy.start()
    for i in range(n_chunk):
        block(q_buf, q_out, q_sem, i)[1].wait()
        block(k_buf, k_out, k_sem, i)[1].wait()
    ratio_copy.wait()


def exchanged(sizes, q_latent, kv_latent, segment_ids, q_weight, k_weight):
    n_dp, n_sec = sizes
    _, length, d_q = q_latent.shape
    rows = q_weight.shape[1]
    heads = k_weight.shape[2] // NOPE
    group = heads // n_dp
    n_pair = group // 2
    bf16, dma = jnp.bfloat16, pltpu.SemaphoreType.DMA
    n_all = n_dp * n_sec
    table = pl.pallas_call(
        functools.partial(maxima_kernel, n_sec),
        out_shape=jax.ShapeDtypeStruct((n_all, group, LANES), jnp.float32),
        in_specs=[pl.BlockSpec(memory_space=pltpu.HBM)] * 6,
        out_specs=pl.BlockSpec(memory_space=pltpu.VMEM),
        scratch_shapes=[
            pltpu.VMEM((n_dp, length, d_q), bf16),
            pltpu.VMEM((n_dp, D_KV + ROPE, length), bf16),
            pltpu.VMEM((n_dp, 1, length), jnp.int32),
            pltpu.VMEM((n_pair, d_q, 2 * HEAD), bf16),
            pltpu.VMEM((D_KV, group * NOPE), bf16),
            pltpu.VMEM((n_dp, n_pair, 2, 2 * NOPE, length), bf16),
            pltpu.VMEM((n_dp, length, length), jnp.float32),
            pltpu.VMEM((group, 8, length), jnp.float32),
            pltpu.VMEM((group, LANES), jnp.float32),
            pltpu.VMEM((n_dp, length, 2 * HEAD), jnp.float32),
            pltpu.VMEM((n_dp, length, LANES), bf16),
            pltpu.VMEM((n_dp, length, LANES), bf16),
            pltpu.VMEM((4, length, LANES), jnp.float32),
            *[pltpu.SemaphoreType.REGULAR] * 4,
            dma,
            dma((n_dp, 2, 2)),
            dma((15, 2)),
            dma((n_dp,)),
            dma((n_dp,)),
            dma((n_pair + 2, n_dp)),
            dma((n_pair + 2, 4)),
            dma,
            dma,
            dma((n_all,)),
            dma((n_all,)),
        ],
        compiler_params=pltpu.CompilerParams(
            collective_id=0, has_side_effects=True, vmem_limit_bytes=VMEM_MIB * 1024 * 1024
        ),
        cost_estimate=pl.CostEstimate(
            flops=2 * n_dp * length * group * (HEAD * (d_q + length) + NOPE * D_KV),
            bytes_accessed=2 * rows * heads * HEAD, transcendentals=0,
        ),
        name="maxima",
    )(
        *[
            pltpu.with_memory_space_constraint(a, pltpu.HBM)
            for a in (
                q_latent[0], kv_latent[0].T, segment_ids.reshape(1, length), q_weight[0],
                k_weight[0], jnp.asarray(rope_tables(length)),
            )
        ],
    )
    ratio, scaled_q, scaled_k = pl.pallas_call(
        functools.partial(scale_kernel, n_sec),
        out_shape=(
            jax.ShapeDtypeStruct((n_sec, heads), jnp.float32),
            jax.ShapeDtypeStruct(q_weight.shape[1:], bf16),
            jax.ShapeDtypeStruct(k_weight.shape[1:], bf16),
        ),
        in_specs=[pl.BlockSpec(memory_space=pltpu.VMEM)] * 3,
        out_specs=[pl.BlockSpec(memory_space=pltpu.HBM)] * 3,
        scratch_shapes=[
            pltpu.VMEM(q_weight.shape[1:], bf16),
            pltpu.VMEM(k_weight.shape[1:], bf16),
            pltpu.VMEM((1, q_weight.shape[2]), jnp.float32),
            pltpu.VMEM((1, k_weight.shape[2]), jnp.float32),
            pltpu.VMEM((n_sec, heads), jnp.float32),
            dma((8,)),
            dma((8,)),
            dma,
        ],
        compiler_params=pltpu.CompilerParams(vmem_limit_bytes=24 * 1024 * 1024),
        cost_estimate=pl.CostEstimate(
            flops=rows * heads * HEAD, bytes_accessed=8 * rows * heads * HEAD, transcendentals=0
        ),
        name="scale",
    )(table, q_weight[0], k_weight[0])
    return ratio, scaled_q[None], scaled_k[None]


def per_device(sizes, q_latent, kv_latent, segment_ids, q_weight, k_weight):
    n_dp, n_sec, n_head = sizes
    heads = k_weight.shape[2] // NOPE
    length = q_latent.shape[1]
    exchange = (
        n_dp == 4 and n_sec % 2 == 0 and q_weight.shape[1] % 384 == 0 and n_head == 2 and heads == 8 * n_dp
        and length % 512 == 0 and q_latent.shape[0] == 1
    )
    args = (q_latent, kv_latent, segment_ids, q_weight, k_weight)
    if exchange:
        return exchanged((n_dp, n_sec), *args)
    own, max_table = gathered_maxima(*args)
    scaled_q, scaled_k = scale_weights(own, q_weight, k_weight)
    return max_table / clip_threshold, scaled_q, scaled_k


def solution(mesh):
    sizes = tuple(mesh.shape[axis] for axis in ("dp", "section", "head"))
    return jax.shard_map(
        functools.partial(per_device, sizes),
        mesh=mesh,
        in_specs=(
            P("section", "dp", None),
            P("section", "dp", None),
            P("dp"),
            P("section", "dp", "head"),
            P("section", None, "head"),
        ),
        out_specs=(P(None, "head"), P("section", "dp", "head"), P("section", None, "head")),
        check_vma=False,
    )
```
